32 devices in a mesh: band: 16 (over z, y, x), chan: 2 (over core).
Axes of the slice: x: 2, y: 2, z: 4, core: 2. Of those that a mesh axis runs over, the one named last changes fastest.
Arguments:
- grid_latent: bfloat16 [18432, 512], P(('band', 'chan')), may hold values from -6 to 6
- edge_latent: bfloat16 [36864, 512], P(('band', 'chan')), may hold values from -6 to 6
- mesh_latent: bfloat16 [5120, 512], P(('band', 'chan')), may hold values from -6 to 6
- mesh_cotangent: bfloat16 [5120, 512], P(('band', 'chan')), may hold values from -6 to 6
- w_grid: bfloat16 [512, 512], P(None, 'chan'), may hold values from -0.15625 to 0.15625
- w_mesh: bfloat16 [512, 512], P(None, 'chan'), may hold values from -0.15625 to 0.15625
- w_edge: bfloat16 [512, 512], P(None, 'chan'), may hold values from -0.15625 to 0.15625
- bias: float32 [512], P('chan'), may hold values from -3 to 3
- w_out: bfloat16 [512, 512], P('chan'), may hold values from -0.25 to 0.25
- senders: int32 [36864], P('band'), may hold values from 0 to 18431, as said below
- receivers: int32 [36864], P('band'), may hold values from 0 to 5119, as said below
- edge_count: int32 [16], P('band'), may hold values from 1152 to 2304, as said below
Outputs:
- grad_grid: bfloat16 [18432, 512], P(('band', 'chan'))
- grad_edge: bfloat16 [36864, 512], P(('band', 'chan'))
- grad_mesh: bfloat16 [5120, 512], P(('band', 'chan'))
- grad_w_grid: float32 [512, 512], P(None, 'chan')
- grad_w_mesh: float32 [512, 512], P(None, 'chan')
- grad_w_edge: float32 [512, 512], P(None, 'chan')
- grad_bias: float32 [512], P('chan')
- grad_w_out: float32 [512, 512], P('chan')
The draws below stay inside these ranges and needn't reach their ends.
Inputs may be any that keep to these rules, and one draw needn't show every extreme that they name: `senders`: an edge of band j (rows j * 2304 to (j + 1) * 2304 - 1) has its sender among grid rows j * 1152 to (j + 1) * 1152 - 1. `receivers`: an edge of band j has its receiver among mesh rows of owners j - 1, j, j + 1 (owner i holds rows i * 320 to (i + 1) * 320 - 1). `edge_count`: some band uses all 2304 slots.
All inputs are finite; a program needn't handle non-finite values.
Results may differ from the reference program's by a relative error of at most 0.0059.
Values may be sent and summed in bfloat16 or wider, within the bound.
A program may use at most 64 MiB of HBM per device.

```python
import jax
import jax.numpy as jnp
from jax import lax

D = 512
H = 512
E_DEV = 2304
MB = 320
G_DEV = 1152
EDGES = 36864
GRID = 18432
MESH = 5120
N_CHAN = 2


def draw_senders(key, part):
    band_of = jnp.arange(EDGES, dtype=jnp.int32) // E_DEV
    return band_of * G_DEV + jax.random.randint(key, (EDGES,), 0, G_DEV, dtype=jnp.int32)


def draw_receivers(key, part):
    first, second = jax.random.split(jax.random.fold_in(key, 11))
    band_of = jnp.arange(EDGES, dtype=jnp.int32) // E_DEV
    offset = jax.random.randint(first, (EDGES,), -1, 2, dtype=jnp.int32)
    owner = jnp.clip(band_of + offset, 0, EDGES // E_DEV - 1)
    return owner * MB + jax.random.randint(second, (EDGES,), 0, MB, dtype=jnp.int32)


def draw_edge_count(key, part):
    first, second = jax.random.split(jax.random.fold_in(key, 23))
    bands = EDGES // E_DEV
    counts = jax.random.randint(first, (bands,), E_DEV // 2, E_DEV + 1, dtype=jnp.int32)
    fullest = jax.random.randint(second, (), 0, bands, dtype=jnp.int32)
    return jnp.where(jnp.arange(bands, dtype=jnp.int32) == fullest, E_DEV, counts)


def steps_of(key, extent, cuts, smallest, top_value):
    factor_of = 1.0
    for position, parts in cuts:
        steps = jax.random.uniform(jax.random.fold_in(jax.random.fold_in(key, 6), position), (parts,), jnp.float32, smallest / len(cuts), top_value / len(cuts))
        factor_of = factor_of * jnp.repeat(jnp.exp(steps), extent[position] // parts).reshape((-1,) + (1,) * (len(extent) - 1 - position))
    return factor_of


def normal_values(stream_key, shape, scale, reach, cuts=(), kind=jnp.bfloat16):
    drawn = jax.random.normal(stream_key, shape, jnp.float32) * scale
    if len(cuts) > 0:
        drawn = steps_of(stream_key, shape, cuts, -0.22, 0.18) * drawn
    return jnp.clip(drawn, min=-reach, max=reach).astype(kind)


def setup_inputs(seed: int = 0) -> dict:
    arg_keys = jax.random.split(jax.random.key(seed), 13)
    return {
        "grid_latent": normal_values(arg_keys[0], (GRID, D), 1.0, 6.0, ((0, 32),)),
        "edge_latent": normal_values(arg_keys[1], (EDGES, D), 1.0, 6.0, ((0, 32),)),
        "mesh_latent": normal_values(arg_keys[2], (MESH, D), 1.0, 6.0, ((0, 32),)),
        "mesh_cotangent": normal_values(arg_keys[3], (MESH, D), 1.0, 6.0, ((0, 32),)),
        "w_grid": normal_values(arg_keys[4], (D, H), (3 * D) ** -0.5, 0.15625, ((1, 2),)),
        "w_mesh": normal_values(arg_keys[5], (D, H), (3 * D) ** -0.5, 0.15625, ((1, 2),)),
        "w_edge": normal_values(arg_keys[6], (D, H), (3 * D) ** -0.5, 0.15625, ((1, 2),)),
        "bias": normal_values(arg_keys[7], (H,), 0.7, 3.0, ((0, 2),), jnp.float32),
        "w_out": normal_values(arg_keys[8], (H, D), H ** -0.5, 0.25, ((0, 2),)),
        "senders": draw_senders(jax.random.fold_in(arg_keys[12], 71), 0),
        "receivers": draw_receivers(jax.random.fold_in(arg_keys[12], 71), 0),
        "edge_count": draw_edge_count(jax.random.fold_in(arg_keys[12], 71), 0),
    }


def reference(grid_latent, edge_latent, mesh_latent, mesh_cotangent, w_grid, w_mesh, w_edge, bias, w_out, senders, receivers, edge_count):
    rows = jnp.arange(EDGES, dtype=jnp.int32)
    live = (rows % E_DEV) < edge_count[rows // E_DEV]
    gsend = grid_latent[senders]
    mrecv = mesh_latent[receivers]
    pre = (jnp.dot(gsend, w_grid, preferred_element_type=jnp.float32)
           + jnp.dot(mrecv, w_mesh, preferred_element_type=jnp.float32)
           + jnp.dot(edge_latent, w_edge, preferred_element_type=jnp.float32) + bias)
    sig = jax.nn.sigmoid(pre)
    act = (pre * sig).astype(jnp.bfloat16)
    message_cot = jnp.where(live[:, None], mesh_cotangent[receivers], jnp.zeros((), jnp.bfloat16))
    hidden_cot = jnp.dot(message_cot, w_out.T, preferred_element_type=jnp.float32)
    pre_cot = (hidden_cot * sig * (1.0 + pre * (1.0 - sig))).astype(jnp.bfloat16)
    grad_w_grid = jnp.dot(gsend.T, pre_cot, preferred_element_type=jnp.float32)
    grad_w_mesh = jnp.dot(mrecv.T, pre_cot, preferred_element_type=jnp.float32)
    grad_w_edge = jnp.dot(edge_latent.T, pre_cot, preferred_element_type=jnp.float32)
    grad_w_out = jnp.dot(act.T, message_cot, preferred_element_type=jnp.float32)
    grad_bias = jnp.sum(pre_cot.astype(jnp.float32), axis=0)
    group = H // N_CHAN
    edge_total = jnp.zeros((EDGES, D), jnp.float32)
    grid_total = jnp.zeros((GRID, D), jnp.float32)
    for index in range(N_CHAN):
        part_cot = pre_cot[:, index * group:(index + 1) * group]
        edge_part = jnp.dot(part_cot, w_edge[:, index * group:(index + 1) * group].T, preferred_element_type=jnp.float32)
        edge_part = lax.optimization_barrier(edge_part.astype(jnp.bfloat16))
        edge_total = edge_total + edge_part.astype(jnp.float32)
        grid_part = jnp.dot(part_cot, w_grid[:, index * group:(index + 1) * group].T, preferred_element_type=jnp.float32)
        grid_part = jax.ops.segment_sum(grid_part, senders, num_segments=GRID)
        grid_part = lax.optimization_barrier(grid_part.astype(jnp.bfloat16))
        grid_total = grid_total + grid_part.astype(jnp.float32)
    mesh_terms = jnp.dot(pre_cot, w_mesh.T, preferred_element_type=jnp.float32)
    grad_mesh = jax.ops.segment_sum(mesh_terms, receivers, num_segments=MESH).astype(jnp.bfloat16)
    return (grid_total.astype(jnp.bfloat16), edge_total.astype(jnp.bfloat16), grad_mesh,
            grad_w_grid, grad_w_mesh, grad_w_edge, grad_bias, grad_w_out)
```

```python
import functools

import jax
import jax.numpy as jnp
from jax import lax
from jax.experimental import pallas as pl
from jax.experimental.pallas import tpu as pltpu
from jax.sharding import PartitionSpec as P

BF = jnp.bfloat16
F32 = jnp.float32
MESH = pl.DeviceIdType.MESH
VMEM = pl.BlockSpec(memory_space=pltpu.VMEM)
ANY = pl.BlockSpec(memory_space=pl.ANY)
NN = (((1,), (0,)), ((), ()))
NT = (((1,), (1,)), ((), ()))
TN = (((0,), (0,)), ((), ()))
WO, WE, WM, WG = range(4)


def mm(a, b, dims=NN):
    return lax.dot_general(a, b, dims, preferred_element_type=F32)


def remote(src, dst, send, recv, device):
    return pltpu.make_async_remote_copy(
        src_ref=src, dst_ref=dst, send_sem=send, recv_sem=recv,
        device_id=device, device_id_type=MESH,
    )


def turned(x):
    return x.astype(F32).T.astype(BF)


def mega_kernel(
    low, high, tile,
    used, grid, edge, mesh, cot, wg, we, wm, wo, bias, sender, receiver,
    edge_out, grid_out, mesh_out, out, bias_out,
    gridv, xv, win, wgv, wev, wmv, wov, biasv, senderv, receiverv,
    wg_t, we_t, s_t, r_t, pg, pm, pre_v, act_v, pc_v, rsum,
    ge_v, ge_in, gg_v, gg_in, rx, rims, gm_v, gm_in,
    gall, in1, sum1, in2, sum2, out1, outv, gb_own, gb_in, gb_sum, gb_all, gb_out,
    local, send, recv, s1, r1, s2, r2, s3, r3, s4, r4, sb, rb, sc, rc,
):
    n = low * high
    me, half = lax.axis_index("band"), lax.axis_index("chan")
    mine, plane = lax.rem(me, low), me // low
    up, down = lax.rem(me + 1, n), lax.rem(me + n - 1, n)
    partner = {"band": me, "chan": 1 - half}
    above, below = {"band": up, "chan": half}, {"band": down, "chan": half}
    rows_g, width = grid.shape
    rows_e, rows_m = edge.shape[0], mesh.shape[0]
    hidden = wg.shape[1]
    own_m = 2 * rows_m
    window = 3 * own_m
    padded = r_t.shape[0]
    edges = 2 * rows_e
    tiles = edges // tile

    barrier = pltpu.get_barrier_semaphore()

    def greet(k, carry):
        pl.semaphore_signal(
            barrier, inc=1, device_id={"band": lax.rem(me + k, n), "chan": half},
            device_id_type=MESH)
        return carry
    pl.semaphore_signal(barrier, inc=1, device_id=partner, device_id_type=MESH)
    lax.fori_loop(1, n, greet, 0)

    loads = [
        pltpu.make_async_copy(src, dst, local.at[i])
        for i, (src, dst) in enumerate((
            (mesh, win.at[0, 1, half]), (cot, win.at[1, 1, half]),
            (grid, gridv.at[half]), (edge, xv.at[half]),
            (wg, wgv), (we, wev), (wm, wmv), (wo, wov), (bias, biasv),
            (sender, senderv), (receiver, receiverv),
        ))
    ]
    for copy in loads:
        copy.start()

    def peer(k):
        return {"band": plane * low + lax.rem(mine + k, low), "chan": half}

    def far(k):
        return {"band": lax.rem(plane + k, high) * low + mine, "chan": half}

    lows, highs = range(1, low), range(1, high)

    def scatter_low(k, w):
        return remote(gall.at[w, lax.rem(mine + k, low)], in1.at[w, k], s1.at[w, k], r1.at[w, k],
                      peer(k))

    def scatter_high(k, w):
        return remote(sum1.at[w, lax.rem(plane + k, high)], in2.at[w, k], s2.at[w, k],
                      r2.at[w, k], far(k))

    def gather_high(k, w):
        return remote(sum2.at[w], out1.at[w, plane], s3.at[w, k], r3.at[w, k], far(k))

    def gather_low(k, w):
        return remote(out1.at[w], out.at[w, mine], s4.at[w, k], r4.at[w, k], peer(k))

    def bias_low(k):
        return remote(gb_own, gb_in.at[mine], sb.at[k], rb.at[k], peer(k))

    def bias_high(k):
        return remote(gb_sum, gb_all.at[plane], sc.at[k], rc.at[k], far(k))

    def offer(w, value):
        gall[w] = value.reshape(gall.shape[1:]).astype(BF)
        for k in lows:
            scatter_low(k, w).start()

    def reduce_low(w):
        for k in lows:
            scatter_low(k, w).wait()
        total = gall[w, mine].astype(F32)
        for k in lows:
            total = total + in1[w, k].astype(F32)
        sum1[w] = total.astype(BF)
        for k in highs:
            scatter_high(k, w).start()

    def reduce_high(w):
        for k in highs:
            scatter_high(k, w).wait()
        total = sum1[w, plane].astype(F32)
        for k in highs:
            total = total + in2[w, k].astype(F32)
        sum2[w] = total.astype(BF)
        for k in highs:
            gather_high(k, w).start()
        out1[w, plane] = sum2[w]

    own_out = [
        pltpu.make_async_copy(out1.at[w], out.at[w, mine], local.at[16 + w]) for w in range(4)
    ]

    def spread(w):
        for k in highs:
            gather_high(k, w).wait()
        for k in lows:
            gather_low(k, w).start()
        own_out[w].start()

    for copy in loads:
        copy.wait()
    wg_t[...] = turned(wgv[...])
    we_t[...] = turned(wev[...])
    bcol = jnp.broadcast_to(biasv[...].reshape(1, hidden), (128, hidden)).T[:, :1]
    pl.semaphore_wait(barrier, n)

    def to_side(which, side, device, i):
        src = win.at[which, 1, half]
        return remote(src, win.at[which, side, half], send.at[i], recv.at[i], device)

    def swap(ref, i):
        return remote(ref.at[half], ref.at[half], send.at[i], recv.at[i], partner)

    mesh_up, mesh_down = to_side(0, 0, above, 0), to_side(0, 2, below, 1)
    cot_up, cot_down = to_side(1, 0, above, 2), to_side(1, 2, below, 3)
    grid_swap, edge_swap = swap(gridv, 4), swap(xv, 5)
    mesh_swap, cot_swap = swap(win.at[0, 1], 6), swap(win.at[1, 1], 7)
    for copy in (mesh_up, mesh_down, grid_swap, edge_swap, mesh_swap, cot_up, cot_down, cot_swap):
        copy.start()

    def pass_on(which, side, i):
        return swap(win.at[which, side], i)

    mesh_on = (pass_on(0, 0, 8), pass_on(0, 2, 9))
    cot_on = (pass_on(1, 0, 10), pass_on(1, 2, 11))

    band_row, mesh_row = me * (2 * rows_g), (me - 1) * own_m
    cuts = [slice(t * tile, (t + 1) * tile) for t in range(tiles)]
    for cut in cuts:
        from_row = senderv[cut].reshape(1, tile) - band_row
        to_row = receiverv[cut].reshape(1, tile) - mesh_row
        s_t[:, cut] = jnp.where(
            lax.broadcasted_iota(jnp.int32, (2 * rows_g, tile), 0) == from_row, 1.0, 0.0
        ).astype(BF)
        r_t[:, cut] = jnp.where(
            lax.broadcasted_iota(jnp.int32, (padded, tile), 0) == to_row, 1.0, 0.0
        ).astype(BF)

    grid_swap.wait()
    grid_all = lambda: gridv[...].reshape(2 * rows_g, width)
    pg[...] = mm(wg_t[...], grid_all(), NT).astype(BF)
    edge_swap.wait()
    x_all = lambda: xv[...].reshape(edges, width)
    for cut in cuts:
        pre_v[:, cut] = mm(pg[...], s_t[:, cut]) + mm(we_t[...], x_all()[cut], NT) + bcol

    def nodes(which):
        rows_in = win[which].reshape(window, width)
        if padded > window:
            rows_in = jnp.concatenate(
                [rows_in, jnp.zeros((padded - window, width), BF)], axis=0)
        return rows_in

    mesh_up.wait()
    mesh_on[0].start()
    mesh_down.wait()
    mesh_on[1].start()
    mesh_swap.wait()
    for copy in mesh_on:
        copy.wait()
    pm[...] = mm(nodes(0), wmv[...]).T.astype(BF)
    count = used[0]
    alive = [
        jnp.where(lax.broadcasted_iota(jnp.int32, (1, tile), 1) + t * tile < count, 1.0, 0.0)
        for t in range(tiles)
    ]
    for t, cut in enumerate(cuts):
        pre = pre_v[:, cut] + mm(pm[...], r_t[:, cut])
        sig = jax.nn.sigmoid(pre)
        act_v[:, cut] = (pre * sig * alive[t]).astype(BF)
        pre_v[:, cut] = sig * (1.0 + pre * (1.0 - sig)) * alive[t]
    rsum[...] = mm(act_v[...], r_t[...], NT).astype(BF)

    cot_up.wait()
    cot_on[0].start()
    cot_down.wait()
    cot_on[1].start()
    cot_swap.wait()
    for copy in cot_on:
        copy.wait()
    offer(WO, mm(rsum[...], nodes(1)))
    pm[...] = mm(wov[...], nodes(1), NT).astype(BF)
    for cut in cuts:
        pc_v[:, cut] = (mm(pm[...], r_t[:, cut]) * pre_v[:, cut]).astype(BF)
    offer(WE, mm(pc_v[...], x_all()))

    gb = jnp.zeros((hidden, 128), F32)
    for k in range(edges // 128):
        gb = gb + pc_v[:, k * 128:(k + 1) * 128].astype(F32)
    gb_own[...] = jnp.broadcast_to(jnp.sum(gb.T, axis=0, keepdims=True), gb_own.shape)
    for k in lows:
        bias_low(k).start()

    sr = mm(pc_v[...], r_t[...], NT)
    offer(WM, mm(sr.astype(BF), nodes(0)))
    rx[...] = sr.T[:window].astype(BF).reshape(rx.shape)
    raise_up = remote(rx.at[2], rims.at[0], send.at[12], recv.at[12], above)
    lower = remote(rx.at[0], rims.at[1], send.at[13], recv.at[13], below)

    sg = mm(pc_v[...], s_t[...], NT).astype(BF)
    offer(WG, mm(sg, grid_all()))
    raise_up.start()
    lower.start()
    reduce_low(WO)
    gg_v[...] = mm(sg, wg_t[...], TN).astype(BF).reshape(gg_v.shape)
    grid_copy = remote(gg_v.at[1 - half], gg_in, send.at[14], recv.at[14], partner)
    grid_copy.start()
    reduce_low(WE)
    ge_v[...] = mm(pc_v[...], we_t[...], TN).astype(BF).reshape(ge_v.shape)
    edge_copy = remote(ge_v.at[1 - half], ge_in, send.at[15], recv.at[15], partner)
    edge_copy.start()

    for k in lows:
        bias_low(k).wait()
    gb_in[mine] = gb_own[...]
    gb_sum[...] = jnp.sum(gb_in[...], axis=0)
    for k in highs:
        bias_high(k).start()
    reduce_low(WM)
    reduce_high(WO)
    reduce_low(WG)
    reduce_high(WE)

    def settle(copy, own, other, to, i):
        copy.wait()
        own[half] = (own[half].astype(F32) + other[...].astype(F32)).astype(BF)
        done = pltpu.make_async_copy(own.at[half], to, local.at[i])
        done.start()
        return done

    grid_done = settle(grid_copy, gg_v, gg_in, grid_out, 11)
    spread(WO)
    edge_done = settle(edge_copy, ge_v, ge_in, edge_out, 12)
    reduce_high(WM)
    spread(WE)
    raise_up.wait()
    lower.wait()
    total = (rx[1].astype(F32) + rims[0].astype(F32) + rims[1].astype(F32)).astype(BF)
    gm_v[...] = mm(total, wmv[...], NT).astype(BF).reshape(gm_v.shape)
    mesh_copy = remote(gm_v.at[1 - half], gm_in, send.at[16], recv.at[16], partner)
    mesh_copy.start()
    reduce_high(WG)
    spread(WM)
    for k in highs:
        bias_high(k).wait()
    gb_all[plane] = gb_sum[...]
    gb_out[...] = jnp.sum(gb_all[...], axis=0)
    bias_done = pltpu.make_async_copy(gb_out, bias_out, local.at[14])
    bias_done.start()
    mesh_done = settle(mesh_copy, gm_v, gm_in, mesh_out, 13)
    spread(WG)
    for copy in (grid_done, edge_done, bias_done, mesh_done, *own_out):
        copy.wait()
    for w in range(4):
        for k in lows:
            gather_low(k, w).wait()


def final_kernel(
    grid_sum, edge_sum, mesh_sum, out, bias_sum,
    grad_grid, grad_edge, grad_mesh, gwg, gwm, gwe, gbias, gwo,
):
    grad_grid[...] = grid_sum[...]
    grad_edge[...] = edge_sum[...]
    grad_mesh[...] = mesh_sum[...]
    full = lambda w: out[w].astype(F32).reshape(gwo.shape)
    gwg[...] = full(WG).T
    gwe[...] = full(WE).T
    gwm[...] = full(WM).T
    gwo[...] = full(WO)
    gbias[...] = bias_sum[...][0]


def body(
    grid_latent,
    edge_latent,
    mesh_latent,
    mesh_cotangent,
    w_grid,
    w_mesh,
    w_edge,
    bias,
    w_out,
    senders,
    receivers,
    edge_count,
):
    n = lax.axis_size("band")
    rows_g, width = grid_latent.shape
    rows_e = edge_latent.shape[0]
    rows_m = mesh_latent.shape[0]
    hidden = w_grid.shape[1]
    own_m = 2 * rows_m
    edges = 2 * rows_e
    sds = jax.ShapeDtypeStruct
    dma = pltpu.SemaphoreType.DMA
    vm = pltpu.VMEM

    tile = max(d for d in range(128, 1025, 128) if edges % d == 0)
    padded = -(-3 * own_m // 256) * 256
    low = 1
    while low * low < n:
        low *= 2
    high = n // low
    rows_c = hidden // n
    piece = (rows_c, width)
    grid_sum, edge_sum, mesh_sum, out, bias_sum = (lambda r: (r[1], r[0], r[2], r[3], r[4]))(
        pl.pallas_call(
            functools.partial(mega_kernel, low, high, tile),
            out_shape=(
                sds((rows_e, width), BF), sds((rows_g, width), BF), sds((rows_m, width), BF),
                sds((4, low, high) + piece, BF), sds((8, hidden), F32),
            ),
            in_specs=[pl.BlockSpec(memory_space=pltpu.SMEM)] + [ANY] * 11,
            out_specs=(ANY,) * 5,
            scratch_shapes=[
                vm((2, rows_g, width), BF), vm((2, rows_e, width), BF),
                vm((2, 3, 2, rows_m, width), BF),
                vm((width, hidden), BF), vm((width, hidden), BF), vm((width, hidden), BF),
                vm((hidden, width), BF), vm((hidden,), F32),
                vm((edges,), jnp.int32), vm((edges,), jnp.int32),
                vm((hidden, width), BF), vm((hidden, width), BF),
                vm((2 * rows_g, edges), BF), vm((padded, edges), BF),
                vm((hidden, 2 * rows_g), BF), vm((hidden, padded), BF),
                vm((hidden, edges), F32), vm((hidden, edges), BF), vm((hidden, edges), BF),
                vm((hidden, padded), BF),
                vm((2, rows_e, width), BF), vm((rows_e, width), BF),
                vm((2, rows_g, width), BF), vm((rows_g, width), BF),
                vm((3, own_m, hidden), BF), vm((2, own_m, hidden), BF),
                vm((2, rows_m, width), BF), vm((rows_m, width), BF),
                vm((4, low, high) + piece, BF), vm((4, low, high) + piece, BF),
                vm((4, high) + piece, BF), vm((4, high) + piece, BF), vm((4,) + piece, BF),
                vm((4, high) + piece, BF), vm((8, 128), F32),
                vm((8, hidden), F32), vm((low, 8, hidden), F32), vm((8, hidden), F32),
                vm((high, 8, hidden), F32), vm((8, hidden), F32),
                dma((20,)), dma((17,)), dma((17,)),
                dma((4, low)), dma((4, low)), dma((4, high)), dma((4, high)),
                dma((4, high)), dma((4, high)), dma((4, low)), dma((4, low)),
                dma((low,)), dma((low,)), dma((high,)), dma((high,)),
            ],
            compiler_params=pltpu.CompilerParams(
                collective_id=0, has_side_effects=True, vmem_limit_bytes=60 * 2**20),
        )(
            edge_count, grid_latent, edge_latent, mesh_latent, mesh_cotangent,
            w_grid, w_edge, w_mesh, w_out, bias, senders, receivers,
        )
    )

    rows_of = lambda rows: pl.BlockSpec((rows // 2, width), lambda t: (t, 0))
    turned_spec = pl.BlockSpec((width, hidden // 2), lambda t: (0, t))
    return pl.pallas_call(
        final_kernel,
        grid=(2,),
        in_specs=[
            rows_of(rows_g), rows_of(rows_e), rows_of(rows_m),
            pl.BlockSpec((4, n // 2) + piece, lambda t: (0, t, 0, 0)),
            pl.BlockSpec((8, hidden), lambda t: (0, 0)),
        ],
        out_specs=(
            rows_of(rows_g), rows_of(rows_e), rows_of(rows_m),
            turned_spec, turned_spec, turned_spec,
            pl.BlockSpec((hidden,), lambda t: (0,)), rows_of(hidden),
        ),
        out_shape=(
            sds((rows_g, width), BF), sds((rows_e, width), BF), sds((rows_m, width), BF),
            sds((width, hidden), F32), sds((width, hidden), F32), sds((width, hidden), F32),
            sds((hidden,), F32), sds((hidden, width), F32),
        ),
        compiler_params=pltpu.CompilerParams(dimension_semantics=("arbitrary",)),
    )(grid_sum, edge_sum, mesh_sum, out.reshape((4, n) + piece), bias_sum)


def solution(mesh):
    rows = P(("band", "chan"), None)
    return jax.shard_map(
        body,
        mesh=mesh,
        in_specs=(
            rows, rows, rows, rows,
            P(None, "chan"), P(None, "chan"), P(None, "chan"), P("chan"), P("chan", None),
            P("band"), P("band"), P("band"),
        ),
        out_specs=(
            rows, rows, rows,
            P(None, "chan"), P(None, "chan"), P(None, "chan"), P("chan"), P("chan", None),
        ),
        check_vma=False,
    )
```

```python
import functools

import jax
import jax.numpy as jnp
from jax import lax
from jax.experimental import pallas as pl
from jax.experimental.pallas import tpu as pltpu
from jax.sharding import PartitionSpec as P

BF = jnp.bfloat16
F32 = jnp.float32
MESH = pl.DeviceIdType.MESH
VMEM = pl.BlockSpec(memory_space=pltpu.VMEM)
ANY = pl.BlockSpec(memory_space=pl.ANY)
NN = (((1,), (0,)), ((), ()))
NT = (((1,), (1,)), ((), ()))
TN = (((0,), (0,)), ((), ()))
WO, WE, WM, WG = range(4)
STAGE = (5.0, 4.2, 4.2, 5.0)


def mm(a, b, dims=NN):
    return lax.dot_general(a, b, dims, preferred_element_type=F32)


def remote(src, dst, send, recv, device):
    return pltpu.make_async_remote_copy(
        src_ref=src, dst_ref=dst, send_sem=send, recv_sem=recv,
        device_id=device, device_id_type=MESH,
    )


def turned(x):
    return x.astype(F32).T.astype(BF)


def mega_kernel(
    tile,
    used, grid, edge, mesh, cot, wg, we, wm, wo, bias, sender, receiver,
    edge_out, grid_out, mesh_out, out, bias_out,
    gridv, xv, win, wgv, wev, wmv, wov, biasv, senderv, receiverv,
    wg_t, we_t, s_t, r_t, pg, pm, pre_v, act_v, pc_v, rsum,
    ge_v, ge_in, gg_v, gg_in, rx, rims, rxs, gm_v, gm_in,
    gall, in1, sum1, in2, sum2, out1, gb_own, gb_in, gb_sum, gb_all, gb_out,
    local, send, recv, wins, xr, fr, pr, qr, ws, wr,
):
    n, half = lax.axis_size("band"), lax.axis_index("chan")
    me = lax.axis_index("band")
    cuts_w, high = gall.shape[1], gall.shape[3]
    mine, plane = lax.rem(me, 4), me // 4
    odd = lax.rem(me, 2)
    pair = me + 1 - 2 * odd
    onward = lax.rem(me + 2 - 4 * odd + n, n)
    backward = lax.rem(me - 2 + 4 * odd + n, n)
    at = lambda band: {"band": band, "chan": half}
    partner = {"band": me, "chan": 1 - half}
    rows_g, width = grid.shape
    rows_e, rows_m = edge.shape[0], mesh.shape[0]
    hidden = wg.shape[1]
    own_m = 2 * rows_m
    window = 3 * own_m
    padded = r_t.shape[0]
    edges = 2 * rows_e
    tiles = edges // tile
    steps = win.shape[3]

    barrier = pltpu.get_barrier_semaphore()

    def greet(k, carry):
        pl.semaphore_signal(
            barrier, inc=1, device_id=at(lax.rem(me + k, n)), device_id_type=MESH)
        return carry
    pl.semaphore_signal(barrier, inc=1, device_id=partner, device_id_type=MESH)
    lax.fori_loop(1, n, greet, 0)

    loads = [
        pltpu.make_async_copy(src, dst, local.at[i])
        for i, (src, dst) in enumerate((
            (mesh.reshape(win.shape[3:]), win.at[0, 1, half]),
            (cot.reshape(win.shape[3:]), win.at[1, 1, half]),
            (grid, gridv.at[half]), (edge, xv.at[half]),
            (sender, senderv), (receiver, receiverv),
            (wg, wgv), (we, wev), (wm, wmv), (wo, wov), (bias, biasv),
        ))
    ]
    for copy in loads:
        copy.start()

    def each(lo, hi, fn):
        if hi - lo <= 8:
            for k in range(lo, hi):
                fn(k)
        else:
            lax.fori_loop(lo, hi, lambda k, carry: (fn(k), carry)[1], 0)

    def swap(ref, s, r):
        return remote(ref.at[half], ref.at[half], s, r, partner)

    def pair_copy(v, i):
        return remote(win.at[v, 1, half, i], win.at[v, 2 * odd, half, i],
                      wins.at[v], xr.at[v, i], at(pair))

    def onward_copy(v, i):
        return remote(win.at[v, 2 - 2 * odd, half, i], win.at[v, 2 * odd, half, i],
                      wins.at[v], fr.at[v, i], at(onward))

    def pair_share(v, i):
        ref = win.at[v, 2 - 2 * odd, half, i]
        return remote(ref, ref, wins.at[v], pr.at[v], partner)

    def onward_share(v, i):
        ref = win.at[v, 2 * odd, half, i]
        return remote(ref, ref, wins.at[v], qr.at[v], partner)

    def pass_pair(v, i):
        pair_copy(v, i).wait_recv()
        onward_copy(v, i).start()
        pair_share(v, i).start()

    def pass_onward(v, i):
        onward_copy(v, i).wait_recv()
        onward_share(v, i).start()

    def shared(v):
        for side, sem in ((2 - 2 * odd, pr), (2 * odd, qr)):
            ref = win.at[v, side, 1 - half]
            remote(ref, ref, wins.at[v], sem.at[v], partner).wait_recv()

    grid_swap, edge_swap = swap(gridv, send.at[0], recv.at[0]), swap(xv, send.at[1], recv.at[1])
    mesh_swap = swap(win.at[0, 1], send.at[2], recv.at[2])
    cot_swap = swap(win.at[1, 1], send.at[3], recv.at[3])

    for copy in loads[:4]:
        copy.wait()
    pl.semaphore_wait(barrier, n)
    for v in (0, 1):
        for i in range(steps):
            pair_copy(v, i).start()
    for copy in (grid_swap, mesh_swap, edge_swap, cot_swap):
        copy.start()
    for copy in loads[4:]:
        copy.wait()
    wg_t[...] = turned(wgv[...])
    we_t[...] = turned(wev[...])
    bcol = jnp.broadcast_to(biasv[...].reshape(1, hidden), (128, hidden)).T[:, :1]

    band_row, mesh_row = me * (2 * rows_g), (me - 1) * own_m
    cuts = [slice(t * tile, (t + 1) * tile) for t in range(tiles)]
    for cut in cuts:
        from_row = senderv[cut].reshape(1, tile) - band_row
        to_row = receiverv[cut].reshape(1, tile) - mesh_row
        s_t[:, cut] = jnp.where(
            lax.broadcasted_iota(jnp.int32, (2 * rows_g, tile), 0) == from_row, 1.0, 0.0
        ).astype(BF)
        r_t[:, cut] = jnp.where(
            lax.broadcasted_iota(jnp.int32, (padded, tile), 0) == to_row, 1.0, 0.0
        ).astype(BF)

    todo = [(v, i) for v in (0, 1) for i in range(steps)]
    pass_pair(*todo.pop(0))
    grid_swap.wait()
    grid_all = lambda: gridv[...].reshape(2 * rows_g, width)
    pg[...] = mm(wg_t[...], grid_all(), NT).astype(BF)
    edge_swap.wait()
    x_all = lambda: xv[...].reshape(edges, width)
    for cut in cuts:
        pre_v[:, cut] = mm(pg[...], s_t[:, cut]) + mm(we_t[...], x_all()[cut], NT) + bcol
        if todo:
            pass_pair(*todo.pop(0))
    for item in todo:
        pass_pair(*item)

    def nodes(which):
        rows_in = win[which].reshape(window, width)
        if padded > window:
            rows_in = jnp.concatenate(
                [rows_in, jnp.zeros((padded - window, width), BF)], axis=0)
        return rows_in

    for i in range(steps):
        pass_onward(0, i)
    mesh_swap.wait()
    shared(0)
    pm[...] = mm(nodes(0), wmv[...]).T.astype(BF)
    count = used[0]
    alive = [
        jnp.where(lax.broadcasted_iota(jnp.int32, (1, tile), 1) + t * tile < count, 1.0, 0.0)
        for t in range(tiles)
    ]
    later = list(range(steps))
    for t, cut in enumerate(cuts):
        pre = pre_v[:, cut] + mm(pm[...], r_t[:, cut])
        sig = jax.nn.sigmoid(pre)
        act_v[:, cut] = (pre * sig * alive[t]).astype(BF)
        pre_v[:, cut] = sig * (1.0 + pre * (1.0 - sig)) * alive[t]
        if t >= 1 and later:
            pass_onward(1, later.pop(0))
    rsum[...] = mm(act_v[...], r_t[...], NT).astype(BF)

    for i in later:
        pass_onward(1, i)
    cot_swap.wait()
    shared(1)

    far = lambda k: lax.rem(plane + k, high)
    near = lambda k: lax.rem(mine + k, 4)
    peer = lambda k: at(plane * 4 + near(k))
    distant = lambda k: at(far(k) * 4 + mine)

    def to(stage, w, c, src, dst, device):
        remote(src, dst, ws.at[w, c], wr.at[stage, w, c], device).start()

    def landed(stage, w, c, ref):
        remote(ref, ref, ws.at[w, c], wr.at[stage, w, c], partner).wait()

    def offer(w, value):
        part = width // cuts_w
        for c in range(cuts_w):
            gall[w, c] = value[:, c * part:(c + 1) * part].reshape(gall.shape[2:]).astype(BF)
            for k in (1, 3, 2):
                to(0, w, c, gall.at[w, c, near(k)], in1.at[w, c, k], peer(k))

    def step1(w, c):
        landed(0, w, c, in1.at[w, c, pl.ds(1, 3)])
        total = gall[w, c, mine].astype(F32)
        for k in range(1, 4):
            total = total + in1[w, c, k].astype(F32)
        sum1[w, c] = total.astype(BF)
        each(1, high, lambda k: to(1, w, c, sum1.at[w, c, far(k)], in2.at[w, c, k], distant(k)))

    def step2(w, c):
        landed(1, w, c, in2.at[w, c, pl.ds(1, high - 1)])
        in2[w, c, 0] = sum1[w, c, plane]
        sum2[w, c] = jnp.sum(in2[w, c].astype(F32), axis=0).astype(BF)
        each(1, high, lambda k: to(2, w, c, sum2.at[w, c], out1.at[w, c, plane], distant(k)))
        out1[w, c, plane] = sum2[w, c]

    def step3(w, c):
        landed(2, w, c, in2.at[w, c, pl.ds(1, high - 1)])
        for k in (1, 3, 2):
            to(3, w, c, out1.at[w, c], out.at[w, c, mine], peer(k))
        keep(w, c).start()

    def step4(w, c):
        landed(3, w, c, in1.at[w, c, pl.ds(1, 3)])

    def keep(w, c):
        return pltpu.make_async_copy(out1.at[w, c], out.at[w, c, mine], local.at[15])

    stages = ((step1, STAGE[0]), (step2, STAGE[1]), (step3, STAGE[2]), (step4, STAGE[3]))

    def bias_low(k):
        return remote(gb_own, gb_in.at[k], send.at[4], recv.at[4], peer(k))

    def bias_high(k):
        return remote(gb_sum, gb_all.at[k], send.at[5], recv.at[5], distant(k))

    rx_on = [
        remote(rx.at[2 * odd, i], rims.at[0, i], send.at[9 + i], recv.at[9 + i], at(backward))
        for i in (0, 1)
    ]
    rx_pair = [
        remote(rxs.at[i], rims.at[1, i], send.at[11 + i], recv.at[11 + i], at(pair))
        for i in (0, 1)
    ]
    grid_copy = remote(gg_v.at[1 - half], gg_in, send.at[6], recv.at[6], partner)
    edge_copy = remote(ge_v.at[1 - half], ge_in, send.at[7], recv.at[7], partner)
    mesh_copy = remote(gm_v.at[1 - half], gm_in, send.at[8], recv.at[8], partner)

    def settle(copy, own, other, to, i):
        copy.wait()
        own[half] = (own[half].astype(F32) + other[...].astype(F32)).astype(BF)
        pltpu.make_async_copy(own.at[half], to, local.at[i]).start()

    grid_sum = (grid_copy, gg_v, gg_in, grid_out, 11)
    edge_sum = (edge_copy, ge_v, ge_in, edge_out, 12)
    mesh_sum = (mesh_copy, gm_v, gm_in, mesh_out, 13)
    bias_done = pltpu.make_async_copy(gb_out, bias_out, local.at[14])

    def rx_step1(i):
        rx_on[i].wait()
        rxs[i] = (rx[2 - 2 * odd, i].astype(F32) + rims[0, i].astype(F32)).astype(BF)
        rx_pair[i].start()

    def rx_step2():
        for copy in rx_pair:
            copy.wait()
        total = (rx[1].astype(F32) + rims[1].astype(F32)).astype(BF).reshape(own_m, hidden)
        gm_v[...] = mm(total, wmv[...], NT).astype(BF).reshape(gm_v.shape)
        mesh_copy.start()

    def bias_step1():
        ref = gb_in.at[pl.ds(1, 3)]
        remote(ref, ref, send.at[4], recv.at[4], partner).wait()
        gb_in[0] = gb_own[...]
        gb_sum[...] = jnp.sum(gb_in[...], axis=0)
        each(1, high, lambda k: bias_high(k).start())

    def bias_step2():
        ref = gb_all.at[pl.ds(1, high - 1)]
        remote(ref, ref, send.at[5], recv.at[5], partner).wait()
        gb_all[0] = gb_sum[...]
        gb_out[...] = jnp.sum(gb_all[...], axis=0)
        bias_done.start()

    keepsake = {}

    def make_wo():
        offer(WO, mm(rsum[...], nodes(1)))

    def make_hidden():
        pm[...] = mm(wov[...], nodes(1), NT).astype(BF)
        for cut in cuts:
            pc_v[:, cut] = (mm(pm[...], r_t[:, cut]) * pre_v[:, cut]).astype(BF)

    def make_we():
        offer(WE, mm(pc_v[...], x_all()))

    def make_bias():
        gb = jnp.zeros((hidden, 128), F32)
        for k in range(edges // 128):
            gb = gb + pc_v[:, k * 128:(k + 1) * 128].astype(F32)
        gb_own[...] = jnp.broadcast_to(jnp.sum(gb.T, axis=0, keepdims=True), gb_own.shape)
        for k in range(1, 4):
            bias_low(k).start()

    def make_wm():
        sr = mm(pc_v[...], r_t[...], NT)
        offer(WM, mm(sr.astype(BF), nodes(0)))
        rx[...] = sr.T[:window].astype(BF).reshape(rx.shape)

    def make_wg():
        keepsake["sg"] = mm(pc_v[...], s_t[...], NT).astype(BF)
        offer(WG, mm(keepsake["sg"], grid_all()))

    def make_grid():
        gg_v[...] = mm(keepsake["sg"], wg_t[...], TN).astype(BF).reshape(gg_v.shape)
        grid_copy.start()

    def make_edge():
        ge_v[...] = mm(pc_v[...], we_t[...], TN).astype(BF).reshape(ge_v.shape)
        edge_copy.start()

    PLAN = (
        (8.2, "rx0a", lambda now: rx_on[0].start()),
        (8.2, "rx0b", lambda now: rx_on[1].start()),
        (12.5, "rx1a", lambda now: rx_step1(0)),
        (14.0, "rx1b", lambda now: rx_step1(1)),
        (15.0, "bias1", lambda now: bias_step1()),
        (12.0, "set_grid", lambda now: settle(*grid_sum)),
        (13.0, "set_edge", lambda now: settle(*edge_sum)),
        (18.0, "rx2", lambda now: rx_step2()),
        (20.5, "set_mesh", lambda now: settle(*mesh_sum)),
        (19.0, "bias2", lambda now: bias_step2()),
    )
    events = []

    def plan(time, name, fn):
        events.append((time, len(events), name, fn))

    def chain(time, w, c, stage):
        fn, lasts = stages[stage]

        def run(now):
            fn(w, c)
            if stage < len(stages) - 1:
                chain(max(now, time + lasts), w, c, stage + 1)
        plan(time + lasts, f"s{stage + 1}_{w}{c}", run)

    def due(now):
        while events and min(events)[0] <= now:
            event = min(events)
            events.remove(event)
            event[3](max(now, event[0]) if now < 1e6 else event[0])

    def offered(w):
        return lambda now: [chain(now, w, c, 0) for c in range(cuts_w)]

    now = 0.0
    for name, fn, lasts, after in (
        ("gwo", make_wo, 0.4, offered(WO)),
        ("hid", make_hidden, 1.8, None),
        ("gwe", make_we, 0.8, offered(WE)),
        ("sr", make_wm, 1.7, offered(WM)),
        ("sg", make_wg, 2.7, offered(WG)),
        ("bias", make_bias, 0.2, None),
        ("gradgrid", make_grid, 0.5, None),
        ("gradedge", make_edge, 0.8, None),
    ):
        due(now)
        fn()
        now += lasts
        if after is not None:
            after(now)
    for time, name, fn in PLAN:
        plan(time, name, fn)
    due(1e9)
    for copy, own, _, to, i in (grid_sum, edge_sum, mesh_sum):
        pltpu.make_async_copy(own.at[half], to, local.at[i]).wait()
    bias_done.wait()
    kept = out1.at[...]
    pltpu.make_async_copy(kept, kept, local.at[15]).wait()
    for v in (0, 1):
        ref = win.at[v, pl.ds(0, 2)]
        remote(ref, ref, wins.at[v], pr.at[v], partner).wait_send()


def final_kernel(
    grid_sum, edge_sum, mesh_sum, out, bias_sum,
    grad_grid, grad_edge, grad_mesh, gwg, gwm, gwe, gbias, gwo,
):
    grad_grid[...] = grid_sum[...]
    grad_edge[...] = edge_sum[...]
    grad_mesh[...] = mesh_sum[...]
    cuts = range(out.shape[1])
    full = lambda w: jnp.concatenate(
        [out[w, c].astype(F32).reshape(gwo.shape[0], -1) for c in cuts], axis=1)
    gwg[...] = full(WG).T
    gwe[...] = full(WE).T
    gwm[...] = full(WM).T
    gwo[...] = full(WO)
    gbias[...] = bias_sum[...][0]


def body(
    grid_latent,
    edge_latent,
    mesh_latent,
    mesh_cotangent,
    w_grid,
    w_mesh,
    w_edge,
    bias,
    w_out,
    senders,
    receivers,
    edge_count,
):
    n = lax.axis_size("band")
    rows_g, width = grid_latent.shape
    rows_e = edge_latent.shape[0]
    rows_m = mesh_latent.shape[0]
    hidden = w_grid.shape[1]
    own_m = 2 * rows_m
    edges = 2 * rows_e
    sds = jax.ShapeDtypeStruct
    dma = pltpu.SemaphoreType.DMA
    vm = pltpu.VMEM

    tile = max(d for d in range(128, 1025, 128) if edges % d == 0)
    padded = -(-3 * own_m // 256) * 256
    high = n // 4
    rows_c = hidden // n
    cuts_w, steps = 2, 2
    piece = (rows_c, width // cuts_w)
    edge_sum, grid_sum, mesh_sum, out, bias_sum = pl.pallas_call(
        functools.partial(mega_kernel, tile),
        out_shape=(
            sds((rows_e, width), BF), sds((rows_g, width), BF), sds((rows_m, width), BF),
            sds((4, cuts_w, 4, high) + piece, BF), sds((8, hidden), F32),
        ),
        in_specs=[pl.BlockSpec(memory_space=pltpu.SMEM)] + [ANY] * 11,
        out_specs=(ANY,) * 5,
        scratch_shapes=[
            vm((2, rows_g, width), BF), vm((2, rows_e, width), BF),
            vm((2, 3, 2, steps, rows_m // steps, width), BF),
            vm((width, hidden), BF), vm((width, hidden), BF), vm((width, hidden), BF),
            vm((hidden, width), BF), vm((hidden,), F32),
            vm((edges,), jnp.int32), vm((edges,), jnp.int32),
            vm((hidden, width), BF), vm((hidden, width), BF),
            vm((2 * rows_g, edges), BF), vm((padded, edges), BF),
            vm((hidden, 2 * rows_g), BF), vm((hidden, padded), BF),
            vm((hidden, edges), F32), vm((hidden, edges), BF), vm((hidden, edges), BF),
            vm((hidden, padded), BF),
            vm((2, rows_e, width), BF), vm((rows_e, width), BF),
            vm((2, rows_g, width), BF), vm((rows_g, width), BF),
            vm((3, 2, rows_m, hidden), BF), vm((2, 2, rows_m, hidden), BF),
            vm((2, rows_m, hidden), BF),
            vm((2, rows_m, width), BF), vm((rows_m, width), BF),
            vm((4, cuts_w, 4, high) + piece, BF), vm((4, cuts_w, 4, high) + piece, BF),
            vm((4, cuts_w, high) + piece, BF), vm((4, cuts_w, high) + piece, BF),
            vm((4, cuts_w) + piece, BF), vm((4, cuts_w, high) + piece, BF),
            vm((8, hidden), F32), vm((4, 8, hidden), F32), vm((8, hidden), F32),
            vm((high, 8, hidden), F32), vm((8, hidden), F32),
            dma((16,)), dma((13,)), dma((13,)),
            dma((2,)), dma((2, steps)), dma((2, steps)), dma((2,)), dma((2,)),
            dma((4, cuts_w)), dma((4, 4, cuts_w)),
        ],
        compiler_params=pltpu.CompilerParams(
            collective_id=0, has_side_effects=True, vmem_limit_bytes=60 * 2**20),
    )(
        edge_count, grid_latent, edge_latent, mesh_latent, mesh_cotangent,
        w_grid, w_edge, w_mesh, w_out, bias, senders, receivers,
    )

    rows_of = lambda rows: pl.BlockSpec((rows // 2, width), lambda t: (t, 0))
    turned_spec = pl.BlockSpec((width, hidden // 2), lambda t: (0, t))
    return pl.pallas_call(
        final_kernel,
        grid=(2,),
        in_specs=[
            rows_of(rows_g), rows_of(rows_e), rows_of(rows_m),
            pl.BlockSpec((4, cuts_w, n // 2) + piece, lambda t: (0, 0, t, 0, 0)),
            pl.BlockSpec((8, hidden), lambda t: (0, 0)),
        ],
        out_specs=(
            rows_of(rows_g), rows_of(rows_e), rows_of(rows_m),
            turned_spec, turned_spec, turned_spec,
            pl.BlockSpec((hidden,), lambda t: (0,)), rows_of(hidden),
        ),
        out_shape=(
            sds((rows_g, width), BF), sds((rows_e, width), BF), sds((rows_m, width), BF),
            sds((width, hidden), F32), sds((width, hidden), F32), sds((width, hidden), F32),
            sds((hidden,), F32), sds((hidden, width), F32),
        ),
        compiler_params=pltpu.CompilerParams(dimension_semantics=("arbitrary",)),
    )(grid_sum, edge_sum, mesh_sum, out.reshape((4, cuts_w, n) + piece), bias_sum)


def solution(mesh):
    rows = P(("band", "chan"), None)
    return jax.shard_map(
        body,
        mesh=mesh,
        in_specs=(
            rows, rows, rows, rows,
            P(None, "chan"), P(None, "chan"), P(None, "chan"), P("chan"), P("chan", None),
            P("band"), P("band"), P("band"),
        ),
        out_specs=(
            rows, rows, rows,
            P(None, "chan"), P(None, "chan"), P(None, "chan"), P("chan"), P("chan", None),
        ),
        check_vma=False,
    )
```

```python
import functools

import jax
import jax.numpy as jnp
from jax import lax
from jax.experimental import pallas as pl
from jax.experimental.pallas import tpu as pltpu
from jax.sharding import PartitionSpec as P

BF = jnp.bfloat16
F32 = jnp.float32
MESH = pl.DeviceIdType.MESH
VMEM = pl.BlockSpec(memory_space=pltpu.VMEM)
ANY = pl.BlockSpec(memory_space=pl.ANY)
NN = (((1,), (0,)), ((), ()))
NT = (((1,), (1,)), ((), ()))
TN = (((0,), (0,)), ((), ()))
WO, WE, WM, WG = range(4)
SPLIT = ()
STAGE = (0.0, 4.2, 4.2, 4.4, 6.0)


def mm(a, b, dims=NN):
    return lax.dot_general(a, b, dims, preferred_element_type=F32)


def remote(src, dst, send, recv, device):
    return pltpu.make_async_remote_copy(
        src_ref=src, dst_ref=dst, send_sem=send, recv_sem=recv,
        device_id=device, device_id_type=MESH,
    )


def turned(x):
    return x.astype(F32).T.astype(BF)


def mega_kernel(
    tile,
    used, grid, edge, mesh, cot, wg, we, wm, wo, bias, sender, receiver,
    edge_out, grid_out, mesh_out, out, bias_out,
    gridv, xv, win, wgv, wev, wmv, wov, biasv, senderv, receiverv,
    wg_t, we_t, s_t, r_t, pg, pm, pc, pre_v, hid_v, act_v, pc_v, sg, rsum,
    ge_v, ge_in, gg_v, gg_in, rx, rims, rxs, gm_v, gm_in,
    gall, in1, sum1, in2, sum2, out1, gb_own, gb_in, gb_sum, gb_all, gb_out,
    local, send, recv, wins, xr, fr, pr, qr, ws, wr,
):
    n, half = lax.axis_size("band"), lax.axis_index("chan")
    me = lax.axis_index("band")
    cuts_w, high = gall.shape[1], gall.shape[3]
    mine, plane = lax.rem(me, 4), me // 4
    bits = (lax.rem(me, 2), lax.rem(me // 2, 2))
    odd = bits[0]
    pair = me + 1 - 2 * odd
    onward = lax.rem(me + 2 - 4 * odd + n, n)
    backward = lax.rem(me - 2 + 4 * odd + n, n)
    at = lambda band: {"band": band, "chan": half}
    partner = {"band": me, "chan": 1 - half}
    rows_g, width = grid.shape
    rows_e, rows_m = edge.shape[0], mesh.shape[0]
    hidden = wg.shape[1]
    own_m = 2 * rows_m
    window = 3 * own_m
    padded = r_t.shape[0]
    edges = 2 * rows_e
    tiles = edges // tile
    steps = win.shape[3]

    barrier = pltpu.get_barrier_semaphore()

    def greet(k, carry):
        pl.semaphore_signal(
            barrier, inc=1, device_id=at(lax.rem(me + k, n)), device_id_type=MESH)
        return carry
    pl.semaphore_signal(barrier, inc=1, device_id=partner, device_id_type=MESH)
    lax.fori_loop(1, n, greet, 0)

    loads = [
        pltpu.make_async_copy(src, dst, local.at[i])
        for i, (src, dst) in enumerate((
            (mesh.reshape(win.shape[3:]), win.at[0, 0, half]),
            (cot.reshape(win.shape[3:]), win.at[1, 0, half]),
            (grid, gridv.at[half]), (edge, xv.at[half]),
            (sender, senderv), (receiver, receiverv),
            (wg, wgv), (we, wev), (wm, wmv), (wo, wov), (bias, biasv),
        ))
    ]
    for copy in loads:
        copy.start()

    def each(lo, hi, fn):
        if hi - lo <= 8:
            for k in range(lo, hi):
                fn(k)
        else:
            lax.fori_loop(lo, hi, lambda k, carry: (fn(k), carry)[1], 0)

    def swap(ref, s, r):
        return remote(ref.at[half], ref.at[half], s, r, partner)

    def pair_copy(v, i):
        return remote(win.at[v, 0, half, i], win.at[v, 1, half, i],
                      wins.at[v], xr.at[v, i], at(pair))

    def onward_copy(v, i):
        return remote(win.at[v, 1, half, i], win.at[v, 2, half, i],
                      wins.at[v], fr.at[v, i], at(onward))

    def pair_share(v, i):
        ref = win.at[v, 1, half, i]
        return remote(ref, ref, wins.at[v], pr.at[v], partner)

    def onward_share(v, i):
        ref = win.at[v, 2, half, i]
        return remote(ref, ref, wins.at[v], qr.at[v], partner)

    def pass_pair(v, i):
        pair_copy(v, i).wait_recv()
        onward_copy(v, i).start()
        pair_share(v, i).start()

    def pass_onward(v, i):
        onward_copy(v, i).wait_recv()
        onward_share(v, i).start()

    def shared(v, slot):
        ref, sem = win.at[v, slot, 1 - half], (pr, qr)[slot - 1]
        remote(ref, ref, wins.at[v], sem.at[v], partner).wait_recv()

    grid_swap, edge_swap = swap(gridv, send.at[0], recv.at[0]), swap(xv, send.at[1], recv.at[1])
    mesh_swap = swap(win.at[0, 0], send.at[2], recv.at[2])
    cot_swap = swap(win.at[1, 0], send.at[3], recv.at[3])

    for copy in loads[:2]:
        copy.wait()
    pl.semaphore_wait(barrier, n)
    for v in (0, 1):
        for i in range(steps):
            pair_copy(v, i).start()
    for copy in loads[2:4]:
        copy.wait()
    for copy in (grid_swap, mesh_swap, edge_swap, cot_swap):
        copy.start()
    for copy in loads[4:]:
        copy.wait()
    wg_t[...] = turned(wgv[...])
    we_t[...] = turned(wev[...])
    bcol = jnp.broadcast_to(biasv[...].reshape(1, hidden), (128, hidden)).T[:, :1]

    block, lanes = 256, 128
    counted = lax.broadcasted_iota(jnp.int32, (block, lanes), 0).astype(F32).astype(BF)
    one, zero = jnp.ones((block, lanes), BF), jnp.zeros((block, lanes), BF)

    def mark(ref, row, cut):
        for base in range(0, ref.shape[0], block):
            size = min(block, ref.shape[0] - base)
            local_row = row - base
            local_row = jnp.where((local_row >= 0) & (local_row < size), local_row, -1)
            local_row = local_row.astype(F32).astype(BF)
            for j in range(0, tile, lanes):
                ref[base:base + size, cut.start + j:cut.start + j + lanes] = jnp.where(
                    counted[:size] == local_row[:, j:j + lanes], one[:size], zero[:size])

    band_row, mesh_row = me * (2 * rows_g), me * own_m
    to_below, to_above = own_m * (3 - odd), own_m * odd
    cuts = [slice(t * tile, (t + 1) * tile) for t in range(tiles)]
    for cut in cuts:
        from_row = senderv[cut].reshape(1, tile) - band_row
        to_row = receiverv[cut].reshape(1, tile) - mesh_row
        to_row = to_row + jnp.where(to_row < 0, to_below, jnp.where(to_row >= own_m, to_above, 0))
        mark(s_t, from_row, cut)
        mark(r_t, to_row, cut)

    grid_swap.wait()
    grid_all = lambda: gridv[...].reshape(2 * rows_g, width)
    pg[...] = mm(wg_t[...], grid_all(), NT).astype(BF)
    pass_pair(0, 0)
    edge_swap.wait()
    x_all = lambda: xv[...].reshape(edges, width)
    for t, cut in enumerate(cuts):
        pre_v[:, cut] = mm(pg[...], s_t[:, cut]) + mm(we_t[...], x_all()[cut], NT) + bcol
        if t == 0:
            for i in range(1, steps):
                pass_pair(0, i)

    near_rows, early = 2 * own_m, padded // 2
    assert early <= near_rows

    def nodes(which):
        rows_in = win[which].reshape(window, width)
        if padded > window:
            rows_in = jnp.concatenate(
                [rows_in, jnp.zeros((padded - window, width), BF)], axis=0)
        return rows_in

    def near_nodes(which):
        return win[which, :2].reshape(near_rows, width)

    def last_nodes(which):
        return jnp.concatenate([
            win[which, 2].reshape(own_m, width),
            jnp.zeros((padded - window, width), BF)], axis=0)

    for i in range(steps // 2):
        pass_pair(1, i)
    mesh_swap.wait()
    shared(0, 1)
    pm[:, :near_rows] = mm(near_nodes(0), wmv[...]).T.astype(BF)
    for t, cut in enumerate(cuts):
        pre_v[:, cut] += mm(pm[:, :early], r_t[:early, cut])
        if t == tiles - 2:
            pass_onward(0, 0)
    for i in range(steps // 2, steps):
        pass_pair(1, i)
    for i in range(1, steps):
        pass_onward(0, i)
    cot_swap.wait()
    shared(1, 1)
    pc[:, :near_rows] = mm(wov[...], near_nodes(1), NT).astype(BF)
    for cut in cuts:
        hid_v[:, cut] = mm(pc[:, :early], r_t[:early, cut])
    shared(0, 2)
    pm[:, near_rows:] = mm(last_nodes(0), wmv[...]).T.astype(BF)
    count = used[0]
    alive = [
        jnp.where(lax.broadcasted_iota(jnp.int32, (1, tile), 1) + t * tile < count, 1.0, 0.0)
        for t in range(tiles)
    ]
    later = list(range(steps))
    for t, cut in enumerate(cuts):
        pre = pre_v[:, cut] + mm(pm[:, early:], r_t[early:, cut])
        sig = jax.nn.sigmoid(pre)
        act_v[:, cut] = (pre * sig * alive[t]).astype(BF)
        pre_v[:, cut] = sig * (1.0 + pre * (1.0 - sig)) * alive[t]
        if t == 0:
            pass_onward(1, 0)
    for i in range(1, steps):
        pass_onward(1, i)
    rsum[...] = mm(act_v[...], r_t[...], NT).astype(BF)
    shared(1, 2)

    far = lambda k: lax.rem(plane + k, high)
    near = lambda k: lax.rem(mine + k, 4)
    peer = lambda k: at(plane * 4 + near(k))
    distant = lambda k: at(far(k) * 4 + mine)

    def to(stage, w, c, src, dst, device):
        remote(src, dst, ws.at[w, c], wr.at[stage, w, c], device).start()

    def landed(stage, w, c, ref):
        remote(ref, ref, ws.at[w, c], wr.at[stage, w, c], partner).wait()

    def offer(w, value):
        part = width // cuts_w
        for c in range(cuts_w):
            gall[w, c] = value[:, c * part:(c + 1) * part].reshape(gall.shape[2:]).astype(BF)
            for k in (1, 3, 2):
                to(0, w, c, gall.at[w, c, near(k)], in1.at[w, c, k], peer(k))

    def step1(w, c):
        landed(0, w, c, in1.at[w, c, pl.ds(1, 3)])
        total = gall[w, c, mine].astype(F32)
        for k in range(1, 4):
            total = total + in1[w, c, k].astype(F32)
        sum1[w, c] = total.astype(BF)
        each(1, high, lambda k: to(1, w, c, sum1.at[w, c, far(k)], in2.at[w, c, k], distant(k)))

    def step2(w, c):
        landed(1, w, c, in2.at[w, c, pl.ds(1, high - 1)])
        in2[w, c, 0] = sum1[w, c, plane]
        sum2[w, c] = jnp.sum(in2[w, c].astype(F32), axis=0).astype(BF)
        each(1, high, lambda k: to(2, w, c, sum2.at[w, c], out1.at[w, c, plane], distant(k)))
        out1[w, c, plane] = sum2[w, c]

    def step3(w, c):
        landed(2, w, c, in2.at[w, c, pl.ds(1, high - 1)])
        if w in SPLIT:
            to(3, w, c, out1.at[w, c], in1.at[w, c, 0], along(second(c)))
        else:
            for k in (1, 3, 2):
                to(3, w, c, out1.at[w, c], out.at[w, c, mine], peer(k))
        keep(w, c).start()

    def step4(w, c):
        if w in SPLIT:
            landed(3, w, c, in1.at[w, c, 0])
            to(4, w, c, out1.at[w, c], out.at[w, c, mine], along(first(c)))
            to(4, w, c, in1.at[w, c, 0], out.at[w, c, flipped(second(c))], along(first(c)))
            keep_landed(w, c).start()
        else:
            landed(3, w, c, in1.at[w, c, pl.ds(1, 3)])

    def step5(w, c):
        if w in SPLIT:
            landed(4, w, c, in1.at[w, c, pl.ds(1, 2)])

    first = lambda c: c % 2
    second = lambda c: 1 - c % 2
    shift = lambda bit: (1 - 2 * bits[bit]) * (1 + bit)
    along = lambda bit: at(me + shift(bit))
    flipped = lambda bit: mine + shift(bit)

    def keep_landed(w, c):
        return pltpu.make_async_copy(
            in1.at[w, c, 0], out.at[w, c, flipped(second(c))], local.at[14])

    def keep(w, c):
        return pltpu.make_async_copy(out1.at[w, c], out.at[w, c, mine], local.at[15])

    stages = (step1, step2, step3, step4, step5)

    def bias_low(k):
        return remote(gb_own, gb_in.at[k], send.at[4], recv.at[4], peer(k))

    def bias_high(k):
        return remote(gb_sum, gb_all.at[k], send.at[5], recv.at[5], distant(k))

    parts = range(rx.shape[1])
    rx_on = [
        remote(rx.at[2, i], rims.at[0, i], send.at[9 + i], recv.at[9 + i], at(backward))
        for i in parts
    ]
    rx_pair = [
        remote(rxs.at[i], rims.at[1, i], send.at[3 + 10 + i], recv.at[3 + 10 + i], at(pair))
        for i in parts
    ]
    grid_copy = remote(gg_v.at[1 - half], gg_in, send.at[6], recv.at[6], partner)
    edge_copy = remote(ge_v.at[1 - half], ge_in, send.at[7], recv.at[7], partner)
    mesh_copy = remote(gm_v.at[1 - half], gm_in, send.at[8], recv.at[8], partner)

    def settle(copy, own, other, to, i):
        copy.wait()
        own[half] = (own[half].astype(F32) + other[...].astype(F32)).astype(BF)
        pltpu.make_async_copy(own.at[half], to, local.at[i]).start()

    grid_sum = (grid_copy, gg_v, gg_in, grid_out, 11)
    edge_sum = (edge_copy, ge_v, ge_in, edge_out, 12)
    mesh_sum = (mesh_copy, gm_v, gm_in, mesh_out, 13)
    bias_done = pltpu.make_async_copy(gb_out, bias_out, local.at[16])

    def rx_step1(i):
        rx_on[i].wait()
        rxs[i] = (rx[1, i].astype(F32) + rims[0, i].astype(F32)).astype(BF)
        rx_pair[i].start()

    def rx_step2():
        for copy in rx_pair:
            copy.wait()
        total = (rx[0].astype(F32) + rims[1].astype(F32)).astype(BF).reshape(own_m, hidden)
        gm_v[...] = mm(total, wmv[...], NT).astype(BF).reshape(gm_v.shape)
        mesh_copy.start()

    def bias_step1():
        ref = gb_in.at[pl.ds(1, 3)]
        remote(ref, ref, send.at[4], recv.at[4], partner).wait()
        gb_in[0] = gb_own[...]
        gb_sum[...] = jnp.sum(gb_in[...], axis=0)
        each(1, high, lambda k: bias_high(k).start())

    def bias_step2():
        ref = gb_all.at[pl.ds(1, high - 1)]
        remote(ref, ref, send.at[5], recv.at[5], partner).wait()
        gb_all[0] = gb_sum[...]
        gb_out[...] = jnp.sum(gb_all[...], axis=0)
        bias_done.start()

    def make_wo():
        offer(WO, mm(rsum[...], nodes(1)))

    def make_hidden():
        pc[:, near_rows:] = mm(wov[...], last_nodes(1), NT).astype(BF)
        for cut in cuts:
            hidden_cot = hid_v[:, cut] + mm(pc[:, early:], r_t[early:, cut])
            pc_v[:, cut] = (hidden_cot * pre_v[:, cut]).astype(BF)

    def make_we():
        offer(WE, mm(pc_v[...], x_all()))

    def make_bias():
        gb = jnp.zeros((hidden, 128), F32)
        for k in range(edges // 128):
            gb = gb + pc_v[:, k * 128:(k + 1) * 128].astype(F32)
        gb_own[...] = jnp.broadcast_to(jnp.sum(gb.T, axis=0, keepdims=True), gb_own.shape)
        for k in range(1, 4):
            bias_low(k).start()

    def make_wm():
        sr = mm(pc_v[...], r_t[...], NT)
        offer(WM, mm(sr.astype(BF), nodes(0)))
        rx[...] = sr.T[:window].astype(BF).reshape(rx.shape)

    split = rows_g // 128 * 128 + 128

    def make_sg():
        sg[:, :split] = mm(pc_v[...], s_t[:split], NT).astype(BF)

    def make_wg():
        sg[:, split:] = mm(pc_v[...], s_t[split:], NT).astype(BF)
        offer(WG, mm(sg[...], grid_all()))

    def make_grid():
        gg_v[...] = mm(sg[...], wg_t[...], TN).astype(BF).reshape(gg_v.shape)
        grid_copy.start()

    def make_edge():
        ge_v[...] = mm(pc_v[...], we_t[...], TN).astype(BF).reshape(ge_v.shape)
        edge_copy.start()

    PLAN = (
        (11.1, "rx0a", lambda now: rx_on[0].start()),
        (15.6, "rx1a", lambda now: rx_step1(0)),
        (12.5, "rx0b", lambda now: rx_on[1].start()),
        (16.6, "rx1b", lambda now: rx_step1(1)),
        (13.6, "rx0c", lambda now: rx_on[2].start()),
        (17.8, "rx1c", lambda now: rx_step1(2)),
        (15.0, "rx0d", lambda now: rx_on[3].start()),
        (19.0, "rx1d", lambda now: rx_step1(3)),
        (15.0, "bias1", lambda now: bias_step1()),
        (12.2, "set_grid", lambda now: settle(*grid_sum)),
        (12.3, "set_edge", lambda now: settle(*edge_sum)),
        (24.5, "rx2", lambda now: rx_step2()),
        (26.5, "set_mesh", lambda now: settle(*mesh_sum)),
        (21.5, "bias2", lambda now: bias_step2()),
    )
    events = []

    def plan(time, name, fn):
        events.append((time, len(events), name, fn))

    def chain(time, w, c):
        for fn, lasts in zip(stages, STAGE):
            time = time + lasts
            plan(time, f"{fn.__name__}_{w}{c}", lambda now, fn=fn: fn(w, c))

    def due(now):
        while events and min(events)[0] <= now:
            event = min(events)
            events.remove(event)
            event[3](max(now, event[0]) if now < 1e6 else event[0])

    def offered(w):
        return lambda now: [
            chain(max(now + 2.2, 2.65) + 1.4 * (c + 1) + 0.8 * w, w, c) for c in range(cuts_w)]

    now = 0.0
    for name, fn, lasts, after in (
        ("gwo", make_wo, 0.45, offered(WO)),
        ("hid", make_hidden, 1.2, None),
        ("gwe", make_we, 0.8, offered(WE)),
        ("sr", make_wm, 1.95, offered(WM)),
        ("sg", make_sg, 1.3, None),
        ("gwg", make_wg, 1.3, offered(WG)),
        ("bias", make_bias, 0.2, None),
        ("gradgrid", make_grid, 0.5, None),
        ("gradedge", make_edge, 0.8, None),
    ):
        due(now)
        fn()
        now += lasts
        if after is not None:
            after(now)
    for time, name, fn in PLAN:
        plan(time, name, fn)
    due(1e9)
    for copy, own, _, to, i in (grid_sum, edge_sum, mesh_sum):
        pltpu.make_async_copy(own.at[half], to, local.at[i]).wait()
    bias_done.wait()
    for kept, i in ((out1, 15),):
        pltpu.make_async_copy(kept, kept, local.at[i]).wait()
    for v in (0, 1):
        ref = win.at[v, pl.ds(0, 2)]
        remote(ref, ref, wins.at[v], pr.at[v], partner).wait_send()


def final_kernel(
    grid_sum, edge_sum, mesh_sum, out, bias_sum,
    grad_grid, grad_edge, grad_mesh, gwg, gwm, gwe, gbias, gwo,
    gv, ev, mv, outv, bv, wide, tall, flat, came, went,
):
    rows = ev.shape[0] // 2
    halves = [pl.ds(i * rows, rows) for i in (0, 1)]
    passing = [
        (edge_sum.at[halves[0]], ev.at[halves[0]], grad_edge.at[halves[0]]),
        (edge_sum.at[halves[1]], ev.at[halves[1]], grad_edge.at[halves[1]]),
        (grid_sum, gv, grad_grid), (mesh_sum, mv, grad_mesh),
    ]
    copy = pltpu.make_async_copy
    into = [copy(out.at[w], outv.at[w], came.at[w]) for w in range(4)]
    into.append(copy(bias_sum, bv, came.at[8]))
    take = [copy(src, mid, came.at[4 + i]) for i, (src, mid, _) in enumerate(passing)]
    give = [copy(mid, dst, went.at[4 + i]) for i, (_, mid, dst) in enumerate(passing)]
    done = [
        copy(wide, gwo, went.at[WO]), copy(tall.at[0], gwe, went.at[WE]),
        copy(tall.at[1], gwm, went.at[WM]), copy(tall.at[2], gwg, went.at[WG]),
    ]
    for read in (into[0], take[0], into[1], take[1], into[2], take[2], into[3], take[3], into[4]):
        read.start()
    for w in range(4):
        into[w].wait()
        value = jnp.concatenate([
            outv[w, c].astype(F32).reshape(wide.shape[0], -1) for c in range(outv.shape[1])
        ], axis=1)
        if w == WO:
            wide[...] = value
        else:
            tall[w - 1] = value.T
        done[w].start()
        take[w].wait()
        give[w].start()
    into[4].wait()
    flat[...] = bv[...][0]
    last = copy(flat, gbias, went.at[8])
    last.start()
    for write in done + give + [last]:
        write.wait()


def body(
    grid_latent,
    edge_latent,
    mesh_latent,
    mesh_cotangent,
    w_grid,
    w_mesh,
    w_edge,
    bias,
    w_out,
    senders,
    receivers,
    edge_count,
):
    n = lax.axis_size("band")
    rows_g, width = grid_latent.shape
    rows_e = edge_latent.shape[0]
    rows_m = mesh_latent.shape[0]
    hidden = w_grid.shape[1]
    own_m = 2 * rows_m
    edges = 2 * rows_e
    sds = jax.ShapeDtypeStruct
    dma = pltpu.SemaphoreType.DMA
    vm = pltpu.VMEM

    tile = max(d for d in range(128, 1025, 128) if edges % d == 0)
    padded = -(-3 * own_m // 256) * 256
    high = n // 4
    rows_c = hidden // n
    cuts_w, steps = 2, 2
    piece = (rows_c, width // cuts_w)
    rim = (4, own_m // 4, hidden)
    edge_sum, grid_sum, mesh_sum, out, bias_sum = pl.pallas_call(
        functools.partial(mega_kernel, tile),
        out_shape=(
            sds((rows_e, width), BF), sds((rows_g, width), BF), sds((rows_m, width), BF),
            sds((4, cuts_w, 4, high) + piece, BF), sds((8, hidden), F32),
        ),
        in_specs=[pl.BlockSpec(memory_space=pltpu.SMEM)] + [ANY] * 11,
        out_specs=(ANY,) * 5,
        scratch_shapes=[
            vm((2, rows_g, width), BF), vm((2, rows_e, width), BF),
            vm((2, 3, 2, steps, rows_m // steps, width), BF),
            vm((width, hidden), BF), vm((width, hidden), BF), vm((width, hidden), BF),
            vm((hidden, width), BF), vm((hidden,), F32),
            vm((edges,), jnp.int32), vm((edges,), jnp.int32),
            vm((hidden, width), BF), vm((hidden, width), BF),
            vm((2 * rows_g, edges), BF), vm((padded, edges), BF),
            vm((hidden, 2 * rows_g), BF), vm((hidden, padded), BF), vm((hidden, padded), BF),
            vm((hidden, edges), F32), vm((hidden, edges), F32), vm((hidden, edges), BF), vm((hidden, edges), BF),
            vm((hidden, 2 * rows_g), BF),
            vm((hidden, padded), BF),
            vm((2, rows_e, width), BF), vm((rows_e, width), BF),
            vm((2, rows_g, width), BF), vm((rows_g, width), BF),
            vm((3,) + rim, BF), vm((2,) + rim, BF), vm(rim, BF),
            vm((2, rows_m, width), BF), vm((rows_m, width), BF),
            vm((4, cuts_w, 4, high) + piece, BF), vm((4, cuts_w, 4, high) + piece, BF),
            vm((4, cuts_w, high) + piece, BF), vm((4, cuts_w, high) + piece, BF),
            vm((4, cuts_w) + piece, BF), vm((4, cuts_w, high) + piece, BF),
            vm((8, hidden), F32), vm((4, 8, hidden), F32), vm((8, hidden), F32),
            vm((high, 8, hidden), F32), vm((8, hidden), F32),
            dma((17,)), dma((17,)), dma((17,)),
            dma((2,)), dma((2, steps)), dma((2, steps)), dma((2,)), dma((2,)),
            dma((4, cuts_w)), dma((5, 4, cuts_w)),
        ],
        compiler_params=pltpu.CompilerParams(
            collective_id=0, has_side_effects=True, vmem_limit_bytes=60 * 2**20),
    )(
        edge_count, grid_latent, edge_latent, mesh_latent, mesh_cotangent,
        w_grid, w_edge, w_mesh, w_out, bias, senders, receivers,
    )

    return pl.pallas_call(
        final_kernel,
        in_specs=[ANY] * 5,
        out_specs=(ANY,) * 8,
        out_shape=(
            sds((rows_g, width), BF), sds((rows_e, width), BF), sds((rows_m, width), BF),
            sds((width, hidden), F32), sds((width, hidden), F32), sds((width, hidden), F32),
            sds((hidden,), F32), sds((hidden, width), F32),
        ),
        scratch_shapes=[
            vm((rows_g, width), BF), vm((rows_e, width), BF), vm((rows_m, width), BF),
            vm((4, cuts_w, n) + piece, BF), vm((8, hidden), F32),
            vm((hidden, width), F32), vm((3, width, hidden), F32), vm((hidden,), F32),
            dma((9,)), dma((9,)),
        ],
    )(grid_sum, edge_sum, mesh_sum, out.reshape((4, cuts_w, n) + piece), bias_sum)


def solution(mesh):
    rows = P(("band", "chan"), None)
    return jax.shard_map(
        body,
        mesh=mesh,
        in_specs=(
            rows, rows, rows, rows,
            P(None, "chan"), P(None, "chan"), P(None, "chan"), P("chan"), P("chan", None),
            P("band"), P("band"), P("band"),
        ),
        out_specs=(
            rows, rows, rows,
            P(None, "chan"), P(None, "chan"), P(None, "chan"), P("chan"), P("chan", None),
        ),
        check_vma=False,
    )
```

```python
import functools

import jax
import jax.numpy as jnp
from jax import lax
from jax.experimental import pallas as pl
from jax.experimental.pallas import tpu as pltpu
from jax.sharding import PartitionSpec as P

BF = jnp.bfloat16
F32 = jnp.float32
MESH = pl.DeviceIdType.MESH
VMEM = pl.BlockSpec(memory_space=pltpu.VMEM)
ANY = pl.BlockSpec(memory_space=pl.ANY)
NN = (((1,), (0,)), ((), ()))
NT = (((1,), (1,)), ((), ()))
TN = (((0,), (0,)), ((), ()))
WO, WE, WM, WG = range(4)
SPLIT = ()
STAGE = (0.0, 4.2, 4.2, 4.4, 6.0)


def mm(a, b, dims=NN):
    return lax.dot_general(a, b, dims, preferred_element_type=F32)


def remote(src, dst, send, recv, device):
    return pltpu.make_async_remote_copy(
        src_ref=src, dst_ref=dst, send_sem=send, recv_sem=recv,
        device_id=device, device_id_type=MESH,
    )


def turned(x):
    return x.astype(F32).T.astype(BF)


def mega_kernel(
    tile,
    used, grid, edge, mesh, cot, wg, we, wm, wo, bias, sender, receiver,
    edge_out, grid_out, mesh_out, out, bias_out,
    gridv, xv, win, wgv, wev, wmv, wov, biasv, senderv, receiverv,
    wg_t, we_t, s_t, r_t, pg, pm, pc, pre_v, hid_v, act_v, pc_v, sg, rsum,
    ge_v, ge_in, gg_v, gg_in, rx, rims, rxs, gm_v, gm_in,
    gall, in1, sum1, in2, sum2, out1, gb_own, gb_in, gb_sum, gb_all, gb_out,
    local, send, recv, wins, xr, fr, pr, qr, ws, wr,
):
    n, half = lax.axis_size("band"), lax.axis_index("chan")
    me = lax.axis_index("band")
    cuts_w, high = gall.shape[1], gall.shape[3]
    mine, plane = lax.rem(me, 4), me // 4
    bits = (lax.rem(me, 2), lax.rem(me // 2, 2))
    odd = bits[0]
    pair = me + 1 - 2 * odd
    onward = lax.rem(me + 2 - 4 * odd + n, n)
    backward = lax.rem(me - 2 + 4 * odd + n, n)
    at = lambda band: {"band": band, "chan": half}
    partner = {"band": me, "chan": 1 - half}
    rows_g, width = grid.shape
    rows_e, rows_m = edge.shape[0], mesh.shape[0]
    hidden = wg.shape[1]
    own_m = 2 * rows_m
    window = 3 * own_m
    padded = r_t.shape[0]
    edges = 2 * rows_e
    tiles = edges // tile
    steps = win.shape[3]

    barrier = pltpu.get_barrier_semaphore()

    def greet(k, carry):
        pl.semaphore_signal(
            barrier, inc=1, device_id=at(lax.rem(me + k, n)), device_id_type=MESH)
        return carry
    pl.semaphore_signal(barrier, inc=1, device_id=partner, device_id_type=MESH)
    lax.fori_loop(1, n, greet, 0)

    loads = [
        pltpu.make_async_copy(src, dst, local.at[i])
        for i, (src, dst) in enumerate((
            (mesh.reshape(win.shape[3:]), win.at[0, 0, half]),
            (cot.reshape(win.shape[3:]), win.at[1, 0, half]),
            (grid, gridv.at[half]), (edge, xv.at[half]),
            (sender, senderv), (receiver, receiverv),
            (wg, wgv), (we, wev), (wm, wmv), (wo, wov), (bias, biasv),
        ))
    ]
    for copy in loads:
        copy.start()

    def each(lo, hi, fn):
        if hi - lo <= 8:
            for k in range(lo, hi):
                fn(k)
        else:
            lax.fori_loop(lo, hi, lambda k, carry: (fn(k), carry)[1], 0)

    def swap(ref, s, r):
        return remote(ref.at[half], ref.at[half], s, r, partner)

    def pair_copy(v, i):
        return remote(win.at[v, 0, half, i], win.at[v, 1, half, i],
                      wins.at[v], xr.at[v, i], at(pair))

    def onward_copy(v, i):
        return remote(win.at[v, 1, half, i], win.at[v, 2, half, i],
                      wins.at[v], fr.at[v, i], at(onward))

    def pair_share(v, i):
        ref = win.at[v, 1, half, i]
        return remote(ref, ref, wins.at[v], pr.at[v], partner)

    def onward_share(v, i):
        ref = win.at[v, 2, half, i]
        return remote(ref, ref, wins.at[v], qr.at[v], partner)

    def pass_pair(v, i):
        pair_copy(v, i).wait_recv()
        onward_copy(v, i).start()
        pair_share(v, i).start()

    def pass_onward(v, i):
        onward_copy(v, i).wait_recv()
        onward_share(v, i).start()

    def shared(v, slot):
        ref, sem = win.at[v, slot, 1 - half], (pr, qr)[slot - 1]
        remote(ref, ref, wins.at[v], sem.at[v], partner).wait_recv()

    grid_swap, edge_swap = swap(gridv, send.at[0], recv.at[0]), swap(xv, send.at[1], recv.at[1])
    mesh_swap = swap(win.at[0, 0], send.at[2], recv.at[2])
    cot_swap = swap(win.at[1, 0], send.at[3], recv.at[3])

    for copy in loads[:2]:
        copy.wait()
    pl.semaphore_wait(barrier, n)
    for v in (0, 1):
        for i in range(steps):
            pair_copy(v, i).start()
    for copy in loads[2:4]:
        copy.wait()
    for copy in (grid_swap, mesh_swap, edge_swap, cot_swap):
        copy.start()
    for copy in loads[4:]:
        copy.wait()
    wg_t[...] = turned(wgv[...])
    we_t[...] = turned(wev[...])
    bcol = jnp.broadcast_to(biasv[...].reshape(1, hidden), (128, hidden)).T[:, :1]

    block, lanes = 256, 128
    counted = lax.broadcasted_iota(jnp.int32, (block, lanes), 0).astype(F32).astype(BF)
    one, zero = jnp.ones((block, lanes), BF), jnp.zeros((block, lanes), BF)

    def mark(ref, row, cut):
        for base in range(0, ref.shape[0], block):
            size = min(block, ref.shape[0] - base)
            local_row = row - base
            local_row = jnp.where((local_row >= 0) & (local_row < size), local_row, -1)
            local_row = local_row.astype(F32).astype(BF)
            for j in range(0, tile, lanes):
                ref[base:base + size, cut.start + j:cut.start + j + lanes] = jnp.where(
                    counted[:size] == local_row[:, j:j + lanes], one[:size], zero[:size])

    band_row, mesh_row = me * (2 * rows_g), me * own_m
    to_below, to_above = own_m * (3 - odd), own_m * odd
    cuts = [slice(t * tile, (t + 1) * tile) for t in range(tiles)]
    for cut in cuts:
        from_row = senderv[cut].reshape(1, tile) - band_row
        to_row = receiverv[cut].reshape(1, tile) - mesh_row
        to_row = to_row + jnp.where(to_row < 0, to_below, jnp.where(to_row >= own_m, to_above, 0))
        mark(s_t, from_row, cut)
        mark(r_t, to_row, cut)

    grid_swap.wait()
    grid_all = lambda: gridv[...].reshape(2 * rows_g, width)
    pg[...] = mm(wg_t[...], grid_all(), NT).astype(BF)
    pass_pair(0, 0)
    edge_swap.wait()
    x_all = lambda: xv[...].reshape(edges, width)
    for t, cut in enumerate(cuts):
        pre_v[:, cut] = mm(pg[...], s_t[:, cut]) + mm(we_t[...], x_all()[cut], NT) + bcol
        if t == 0:
            for i in range(1, steps):
                pass_pair(0, i)

    near_rows, early = 2 * own_m, padded // 2
    assert early <= near_rows

    def nodes(which):
        rows_in = win[which].reshape(window, width)
        if padded > window:
            rows_in = jnp.concatenate(
                [rows_in, jnp.zeros((padded - window, width), BF)], axis=0)
        return rows_in

    def near_nodes(which):
        return win[which, :2].reshape(near_rows, width)

    def last_nodes(which):
        return jnp.concatenate([
            win[which, 2].reshape(own_m, width),
            jnp.zeros((padded - window, width), BF)], axis=0)

    for i in range(steps // 2):
        pass_pair(1, i)
    mesh_swap.wait()
    shared(0, 1)
    pm[:, :near_rows] = mm(near_nodes(0), wmv[...]).T.astype(BF)
    for t, cut in enumerate(cuts):
        pre_v[:, cut] += mm(pm[:, :early], r_t[:early, cut])
        if t == tiles - 2:
            pass_onward(0, 0)
            for i in range(steps // 2, steps):
                pass_pair(1, i)
    for i in range(1, steps):
        pass_onward(0, i)
    cot_swap.wait()
    shared(1, 1)
    pc[:, :near_rows] = mm(wov[...], near_nodes(1), NT).astype(BF)
    for cut in cuts:
        hid_v[:, cut] = mm(pc[:, :early], r_t[:early, cut])
    shared(0, 2)
    pm[:, near_rows:] = mm(last_nodes(0), wmv[...]).T.astype(BF)
    count = used[0]
    alive = [
        jnp.where(lax.broadcasted_iota(jnp.int32, (1, tile), 1) + t * tile < count, 1.0, 0.0)
        for t in range(tiles)
    ]
    later = list(range(steps))
    for t, cut in enumerate(cuts):
        pre = pre_v[:, cut] + mm(pm[:, early:], r_t[early:, cut])
        sig = jax.nn.sigmoid(pre)
        act_v[:, cut] = (pre * sig * alive[t]).astype(BF)
        pre_v[:, cut] = sig * (1.0 + pre * (1.0 - sig)) * alive[t]
        if t == 0:
            pass_onward(1, 0)
    for i in range(1, steps):
        pass_onward(1, i)
    rsum[...] = mm(act_v[...], r_t[...], NT).astype(BF)
    shared(1, 2)

    far = lambda k: lax.rem(plane + k, high)
    near = lambda k: lax.rem(mine + k, 4)
    peer = lambda k: at(plane * 4 + near(k))
    distant = lambda k: at(far(k) * 4 + mine)

    def to(stage, w, c, src, dst, device):
        remote(src, dst, ws.at[w, c], wr.at[stage, w, c], device).start()

    def landed(stage, w, c, ref):
        remote(ref, ref, ws.at[w, c], wr.at[stage, w, c], partner).wait()

    def offer(w, value):
        part = width // cuts_w
        for c in range(cuts_w):
            gall[w, c] = value[:, c * part:(c + 1) * part].reshape(gall.shape[2:]).astype(BF)
            for k in (1, 3, 2):
                to(0, w, c, gall.at[w, c, near(k)], in1.at[w, c, k], peer(k))

    def step1(w, c):
        landed(0, w, c, in1.at[w, c, pl.ds(1, 3)])
        total = gall[w, c, mine].astype(F32)
        for k in range(1, 4):
            total = total + in1[w, c, k].astype(F32)
        sum1[w, c] = total.astype(BF)
        each(1, high, lambda k: to(1, w, c, sum1.at[w, c, far(k)], in2.at[w, c, k], distant(k)))

    def step2(w, c):
        landed(1, w, c, in2.at[w, c, pl.ds(1, high - 1)])
        in2[w, c, 0] = sum1[w, c, plane]
        sum2[w, c] = jnp.sum(in2[w, c].astype(F32), axis=0).astype(BF)
        each(1, high, lambda k: to(2, w, c, sum2.at[w, c], out1.at[w, c, plane], distant(k)))
        out1[w, c, plane] = sum2[w, c]

    def step3(w, c):
        landed(2, w, c, in2.at[w, c, pl.ds(1, high - 1)])
        if w in SPLIT:
            to(3, w, c, out1.at[w, c], in1.at[w, c, 0], along(second(c)))
        else:
            for k in (1, 3, 2):
                to(3, w, c, out1.at[w, c], out.at[w, c, mine], peer(k))
        keep(w, c).start()

    def step4(w, c):
        if w in SPLIT:
            landed(3, w, c, in1.at[w, c, 0])
            to(4, w, c, out1.at[w, c], out.at[w, c, mine], along(first(c)))
            to(4, w, c, in1.at[w, c, 0], out.at[w, c, flipped(second(c))], along(first(c)))
            keep_landed(w, c).start()
        else:
            landed(3, w, c, in1.at[w, c, pl.ds(1, 3)])

    def step5(w, c):
        if w in SPLIT:
            landed(4, w, c, in1.at[w, c, pl.ds(1, 2)])

    first = lambda c: c % 2
    second = lambda c: 1 - c % 2
    shift = lambda bit: (1 - 2 * bits[bit]) * (1 + bit)
    along = lambda bit: at(me + shift(bit))
    flipped = lambda bit: mine + shift(bit)

    def keep_landed(w, c):
        return pltpu.make_async_copy(
            in1.at[w, c, 0], out.at[w, c, flipped(second(c))], local.at[14])

    def keep(w, c):
        return pltpu.make_async_copy(out1.at[w, c], out.at[w, c, mine], local.at[15])

    stages = (step1, step2, step3, step4, step5)

    def bias_low(k):
        return remote(gb_own, gb_in.at[k], send.at[4], recv.at[4], peer(k))

    def bias_high(k):
        return remote(gb_sum, gb_all.at[k], send.at[5], recv.at[5], distant(k))

    parts = range(rx.shape[1])
    rx_on = [
        remote(rx.at[2, i], rims.at[0, i], send.at[9 + i], recv.at[9 + i], at(backward))
        for i in parts
    ]
    rx_pair = [
        remote(rxs.at[i], rims.at[1, i], send.at[3 + 10 + i], recv.at[3 + 10 + i], at(pair))
        for i in parts
    ]
    grid_copy = remote(gg_v.at[1 - half], gg_in, send.at[6], recv.at[6], partner)
    edge_copy = remote(ge_v.at[1 - half], ge_in, send.at[7], recv.at[7], partner)
    mesh_copy = remote(gm_v.at[1 - half], gm_in, send.at[8], recv.at[8], partner)

    def settle(copy, own, other, to, i):
        copy.wait()
        own[half] = (own[half].astype(F32) + other[...].astype(F32)).astype(BF)
        pltpu.make_async_copy(own.at[half], to, local.at[i]).start()

    grid_sum = (grid_copy, gg_v, gg_in, grid_out, 11)
    edge_sum = (edge_copy, ge_v, ge_in, edge_out, 12)
    mesh_sum = (mesh_copy, gm_v, gm_in, mesh_out, 13)
    bias_done = pltpu.make_async_copy(gb_out, bias_out, local.at[16])

    def rx_step1(i):
        rx_on[i].wait()
        rxs[i] = (rx[1, i].astype(F32) + rims[0, i].astype(F32)).astype(BF)
        rx_pair[i].start()

    def rx_step2():
        for copy in rx_pair:
            copy.wait()
        total = (rx[0].astype(F32) + rims[1].astype(F32)).astype(BF).reshape(own_m, hidden)
        gm_v[...] = mm(total, wmv[...], NT).astype(BF).reshape(gm_v.shape)
        mesh_copy.start()

    def bias_step1():
        ref = gb_in.at[pl.ds(1, 3)]
        remote(ref, ref, send.at[4], recv.at[4], partner).wait()
        gb_in[0] = gb_own[...]
        gb_sum[...] = jnp.sum(gb_in[...], axis=0)
        each(1, high, lambda k: bias_high(k).start())

    def bias_step2():
        ref = gb_all.at[pl.ds(1, high - 1)]
        remote(ref, ref, send.at[5], recv.at[5], partner).wait()
        gb_all[0] = gb_sum[...]
        gb_out[...] = jnp.sum(gb_all[...], axis=0)
        bias_done.start()

    def make_wo():
        offer(WO, mm(rsum[...], nodes(1)))

    def make_hidden():
        pc[:, near_rows:] = mm(wov[...], last_nodes(1), NT).astype(BF)
        for cut in cuts:
            hidden_cot = hid_v[:, cut] + mm(pc[:, early:], r_t[early:, cut])
            pc_v[:, cut] = (hidden_cot * pre_v[:, cut]).astype(BF)

    def make_we():
        offer(WE, mm(pc_v[...], x_all()))

    def make_bias():
        gb = jnp.zeros((hidden, 128), F32)
        for k in range(edges // 128):
            gb = gb + pc_v[:, k * 128:(k + 1) * 128].astype(F32)
        gb_own[...] = jnp.broadcast_to(jnp.sum(gb.T, axis=0, keepdims=True), gb_own.shape)
        for k in range(1, 4):
            bias_low(k).start()

    def make_wm():
        sr = mm(pc_v[...], r_t[...], NT)
        offer(WM, mm(sr.astype(BF), nodes(0)))
        rx[...] = sr.T[:window].astype(BF).reshape(rx.shape)

    split = rows_g // 128 * 128 + 128

    def make_sg():
        sg[:, :split] = mm(pc_v[...], s_t[:split], NT).astype(BF)

    def make_wg():
        sg[:, split:] = mm(pc_v[...], s_t[split:], NT).astype(BF)
        offer(WG, mm(sg[...], grid_all()))

    def make_grid():
        gg_v[...] = mm(sg[...], wg_t[...], TN).astype(BF).reshape(gg_v.shape)
        grid_copy.start()

    def make_edge():
        ge_v[...] = mm(pc_v[...], we_t[...], TN).astype(BF).reshape(ge_v.shape)
        edge_copy.start()

    PLAN = (
        (11.1, "rx0a", lambda now: rx_on[0].start()),
        (15.6, "rx1a", lambda now: rx_step1(0)),
        (12.5, "rx0b", lambda now: rx_on[1].start()),
        (16.6, "rx1b", lambda now: rx_step1(1)),
        (13.6, "rx0c", lambda now: rx_on[2].start()),
        (17.8, "rx1c", lambda now: rx_step1(2)),
        (15.0, "rx0d", lambda now: rx_on[3].start()),
        (19.0, "rx1d", lambda now: rx_step1(3)),
        (15.0, "bias1", lambda now: bias_step1()),
        (12.2, "set_grid", lambda now: settle(*grid_sum)),
        (12.3, "set_edge", lambda now: settle(*edge_sum)),
        (24.5, "rx2", lambda now: rx_step2()),
        (26.5, "set_mesh", lambda now: settle(*mesh_sum)),
        (21.5, "bias2", lambda now: bias_step2()),
    )
    events = []

    def plan(time, name, fn):
        events.append((time, len(events), name, fn))

    def chain(time, w, c):
        for fn, lasts in zip(stages, STAGE):
            time = time + lasts + (1.5 if fn is step4 and w not in SPLIT else 0.0)
            plan(time, f"{fn.__name__}_{w}{c}", lambda now, fn=fn: fn(w, c))

    def due(now):
        while events and min(events)[0] <= now:
            event = min(events)
            events.remove(event)
            event[3](max(now, event[0]) if now < 1e6 else event[0])

    def offered(w):
        return lambda now: [
            chain(max(now + 2.2, 2.65) + 1.4 * (c + 1) + 0.8 * w, w, c) for c in range(cuts_w)]

    now = 0.0
    for name, fn, lasts, after in (
        ("gwo", make_wo, 0.45, offered(WO)),
        ("hid", make_hidden, 1.2, None),
        ("gwe", make_we, 0.8, offered(WE)),
        ("sr", make_wm, 1.95, offered(WM)),
        ("sg", make_sg, 1.3, None),
        ("gwg", make_wg, 1.3, offered(WG)),
        ("bias", make_bias, 0.2, None),
        ("gradgrid", make_grid, 0.5, None),
        ("gradedge", make_edge, 0.8, None),
    ):
        due(now)
        fn()
        now += lasts
        if after is not None:
            after(now)
    for time, name, fn in PLAN:
        plan(time, name, fn)
    due(1e9)
    for copy, own, _, to, i in (grid_sum, edge_sum, mesh_sum):
        pltpu.make_async_copy(own.at[half], to, local.at[i]).wait()
    bias_done.wait()
    pltpu.make_async_copy(out1, out1, local.at[15]).wait()
    for v in (0, 1):
        ref = win.at[v, pl.ds(0, 2)]
        remote(ref, ref, wins.at[v], pr.at[v], partner).wait_send()


def final_kernel(
    grid_sum, edge_sum, mesh_sum, out, bias_sum,
    grad_grid, grad_edge, grad_mesh, gwg, gwm, gwe, gbias, gwo,
    gv, ev, mv, outv, bv, wide, tall, flat, came, went,
):
    rows = ev.shape[0] // 2
    halves = [pl.ds(i * rows, rows) for i in (0, 1)]
    passing = [
        (edge_sum.at[halves[0]], ev.at[halves[0]], grad_edge.at[halves[0]]),
        (edge_sum.at[halves[1]], ev.at[halves[1]], grad_edge.at[halves[1]]),
        (grid_sum, gv, grad_grid), (mesh_sum, mv, grad_mesh),
    ]
    copy = pltpu.make_async_copy
    into = [copy(out.at[w], outv.at[w], came.at[w]) for w in range(4)]
    into.append(copy(bias_sum, bv, came.at[8]))
    take = [copy(src, mid, came.at[4 + i]) for i, (src, mid, _) in enumerate(passing)]
    give = [copy(mid, dst, went.at[4 + i]) for i, (_, mid, dst) in enumerate(passing)]
    done = [
        copy(wide, gwo, went.at[WO]), copy(tall.at[0], gwe, went.at[WE]),
        copy(tall.at[1], gwm, went.at[WM]), copy(tall.at[2], gwg, went.at[WG]),
    ]
    for read in (into[0], take[0], into[1], take[1], into[2], take[2], into[3], take[3], into[4]):
        read.start()
    for w in range(4):
        into[w].wait()
        value = jnp.concatenate([
            outv[w, c].astype(F32).reshape(wide.shape[0], -1) for c in range(outv.shape[1])
        ], axis=1)
        if w == WO:
            wide[...] = value
        else:
            tall[w - 1] = value.T
        done[w].start()
        take[w].wait()
        give[w].start()
    into[4].wait()
    flat[...] = bv[...][0]
    last = copy(flat, gbias, went.at[8])
    last.start()
    for write in done + give + [last]:
        write.wait()


def body(
    grid_latent,
    edge_latent,
    mesh_latent,
    mesh_cotangent,
    w_grid,
    w_mesh,
    w_edge,
    bias,
    w_out,
    senders,
    receivers,
    edge_count,
):
    n = lax.axis_size("band")
    rows_g, width = grid_latent.shape
    rows_e = edge_latent.shape[0]
    rows_m = mesh_latent.shape[0]
    hidden = w_grid.shape[1]
    own_m = 2 * rows_m
    edges = 2 * rows_e
    sds = jax.ShapeDtypeStruct
    dma = pltpu.SemaphoreType.DMA
    vm = pltpu.VMEM

    tile = max(d for d in range(128, 1025, 128) if edges % d == 0)
    padded = -(-3 * own_m // 256) * 256
    high = n // 4
    rows_c = hidden // n
    cuts_w, steps = 2, 2
    piece = (rows_c, width // cuts_w)
    rim = (4, own_m // 4, hidden)
    edge_sum, grid_sum, mesh_sum, out, bias_sum = pl.pallas_call(
        functools.partial(mega_kernel, tile),
        out_shape=(
            sds((rows_e, width), BF), sds((rows_g, width), BF), sds((rows_m, width), BF),
            sds((4, cuts_w, 4, high) + piece, BF), sds((8, hidden), F32),
        ),
        in_specs=[pl.BlockSpec(memory_space=pltpu.SMEM)] + [ANY] * 11,
        out_specs=(ANY,) * 5,
        scratch_shapes=[
            vm((2, rows_g, width), BF), vm((2, rows_e, width), BF),
            vm((2, 3, 2, steps, rows_m // steps, width), BF),
            vm((width, hidden), BF), vm((width, hidden), BF), vm((width, hidden), BF),
            vm((hidden, width), BF), vm((hidden,), F32),
            vm((edges,), jnp.int32), vm((edges,), jnp.int32),
            vm((hidden, width), BF), vm((hidden, width), BF),
            vm((2 * rows_g, edges), BF), vm((padded, edges), BF),
            vm((hidden, 2 * rows_g), BF), vm((hidden, padded), BF), vm((hidden, padded), BF),
            vm((hidden, edges), F32), vm((hidden, edges), F32), vm((hidden, edges), BF), vm((hidden, edges), BF),
            vm((hidden, 2 * rows_g), BF),
            vm((hidden, padded), BF),
            vm((2, rows_e, width), BF), vm((rows_e, width), BF),
            vm((2, rows_g, width), BF), vm((rows_g, width), BF),
            vm((3,) + rim, BF), vm((2,) + rim, BF), vm(rim, BF),
            vm((2, rows_m, width), BF), vm((rows_m, width), BF),
            vm((4, cuts_w, 4, high) + piece, BF), vm((4, cuts_w, 4, high) + piece, BF),
            vm((4, cuts_w, high) + piece, BF), vm((4, cuts_w, high) + piece, BF),
            vm((4, cuts_w) + piece, BF), vm((4, cuts_w, high) + piece, BF),
            vm((8, hidden), F32), vm((4, 8, hidden), F32), vm((8, hidden), F32),
            vm((high, 8, hidden), F32), vm((8, hidden), F32),
            dma((17,)), dma((17,)), dma((17,)),
            dma((2,)), dma((2, steps)), dma((2, steps)), dma((2,)), dma((2,)),
            dma((4, cuts_w)), dma((5, 4, cuts_w)),
        ],
        compiler_params=pltpu.CompilerParams(
            collective_id=0, has_side_effects=True, vmem_limit_bytes=60 * 2**20),
    )(
        edge_count, grid_latent, edge_latent, mesh_latent, mesh_cotangent,
        w_grid, w_edge, w_mesh, w_out, bias, senders, receivers,
    )

    return pl.pallas_call(
        final_kernel,
        in_specs=[ANY] * 5,
        out_specs=(ANY,) * 8,
        out_shape=(
            sds((rows_g, width), BF), sds((rows_e, width), BF), sds((rows_m, width), BF),
            sds((width, hidden), F32), sds((width, hidden), F32), sds((width, hidden), F32),
            sds((hidden,), F32), sds((hidden, width), F32),
        ),
        scratch_shapes=[
            vm((rows_g, width), BF), vm((rows_e, width), BF), vm((rows_m, width), BF),
            vm((4, cuts_w, n) + piece, BF), vm((8, hidden), F32),
            vm((hidden, width), F32), vm((3, width, hidden), F32), vm((hidden,), F32),
            dma((9,)), dma((9,)),
        ],
    )(grid_sum, edge_sum, mesh_sum, out.reshape((4, cuts_w, n) + piece), bias_sum)


def solution(mesh):
    rows = P(("band", "chan"), None)
    return jax.shard_map(
        body,
        mesh=mesh,
        in_specs=(
            rows, rows, rows, rows,
            P(None, "chan"), P(None, "chan"), P(None, "chan"), P("chan"), P("chan", None),
            P("band"), P("band"), P("band"),
        ),
        out_specs=(
            rows, rows, rows,
            P(None, "chan"), P(None, "chan"), P(None, "chan"), P("chan"), P("chan", None),
        ),
        check_vma=False,
    )
```

```python
import functools

import jax
import jax.numpy as jnp
from jax import lax
from jax.experimental import pallas as pl
from jax.experimental.pallas import tpu as pltpu
from jax.sharding import PartitionSpec as P

BF = jnp.bfloat16
F32 = jnp.float32
MESH = pl.DeviceIdType.MESH
VMEM = pl.BlockSpec(memory_space=pltpu.VMEM)
ANY = pl.BlockSpec(memory_space=pl.ANY)
NN = (((1,), (0,)), ((), ()))
NT = (((1,), (1,)), ((), ()))
TN = (((0,), (0,)), ((), ()))
WO, WE, WM, WG = range(4)
SPLIT = ()
STAGE = (0.0, 4.2, 4.2, 4.4, 6.0)


def mm(a, b, dims=NN):
    return lax.dot_general(a, b, dims, preferred_element_type=F32)


def remote(src, dst, send, recv, device):
    return pltpu.make_async_remote_copy(
        src_ref=src, dst_ref=dst, send_sem=send, recv_sem=recv,
        device_id=device, device_id_type=MESH,
    )


def turned(x):
    return x.astype(F32).T.astype(BF)


def mega_kernel(
    tile,
    used, grid, edge, mesh, cot, wg, we, wm, wo, bias, sender, receiver,
    edge_out, grid_out, mesh_out, out, bias_out,
    gridv, xv, win, wgv, wev, wmv, wov, biasv, senderv, receiverv,
    wg_t, we_t, s_t, r_t, pg, pm, pc, pre_v, hid_v, act_v, pc_v, sg, rsum,
    ge_v, ge_in, gg_v, gg_in, rx, rims, rxs, gm_v, gm_in,
    gall, in1, sum1, in2, sum2, out1, gb_own, gb_in, gb_sum, gb_all, gb_out,
    local, send, recv, wins, xr, fr, pr, qr, ws, wr,
):
    n, half = lax.axis_size("band"), lax.axis_index("chan")
    me = lax.axis_index("band")
    cuts_w, high = gall.shape[1], gall.shape[3]
    mine, plane = lax.rem(me, 4), me // 4
    bits = (lax.rem(me, 2), lax.rem(me // 2, 2))
    odd = bits[0]
    pair = me + 1 - 2 * odd
    onward = lax.rem(me + 2 - 4 * odd + n, n)
    backward = lax.rem(me - 2 + 4 * odd + n, n)
    at = lambda band: {"band": band, "chan": half}
    partner = {"band": me, "chan": 1 - half}
    rows_g, width = grid.shape
    rows_e, rows_m = edge.shape[0], mesh.shape[0]
    hidden = wg.shape[1]
    own_m = 2 * rows_m
    window = 3 * own_m
    padded = r_t.shape[0]
    edges = 2 * rows_e
    tiles = edges // tile
    steps = win.shape[3]

    barrier = pltpu.get_barrier_semaphore()

    def greet(k, carry):
        pl.semaphore_signal(
            barrier, inc=1, device_id=at(lax.rem(me + k, n)), device_id_type=MESH)
        return carry
    pl.semaphore_signal(barrier, inc=1, device_id=partner, device_id_type=MESH)
    lax.fori_loop(1, n, greet, 0)

    loads = [
        pltpu.make_async_copy(src, dst, local.at[i])
        for i, (src, dst) in enumerate((
            (mesh.reshape(win.shape[3:]), win.at[0, 0, half]),
            (cot.reshape(win.shape[3:]), win.at[1, 0, half]),
            (grid, gridv.at[half]), (edge, xv.at[half]),
            (sender, senderv), (receiver, receiverv),
            (wg, wgv), (we, wev), (wm, wmv), (wo, wov), (bias, biasv),
        ))
    ]
    for copy in loads:
        copy.start()

    def each(lo, hi, fn):
        if hi - lo <= 8:
            for k in range(lo, hi):
                fn(k)
        else:
            lax.fori_loop(lo, hi, lambda k, carry: (fn(k), carry)[1], 0)

    def swap(ref, s, r):
        return remote(ref.at[half], ref.at[half], s, r, partner)

    def pair_copy(v, i):
        return remote(win.at[v, 0, half, i], win.at[v, 1, half, i],
                      wins.at[v], xr.at[v, i], at(pair))

    def onward_copy(v, i):
        return remote(win.at[v, 1, half, i], win.at[v, 2, half, i],
                      wins.at[v], fr.at[v, i], at(onward))

    def pair_share(v, i):
        ref = win.at[v, 1, half, i]
        return remote(ref, ref, wins.at[v], pr.at[v], partner)

    def onward_share(v, i):
        ref = win.at[v, 2, half, i]
        return remote(ref, ref, wins.at[v], qr.at[v], partner)

    def pass_pair(v, i):
        pair_copy(v, i).wait_recv()
        onward_copy(v, i).start()
        pair_share(v, i).start()

    def pass_onward(v, i):
        onward_copy(v, i).wait_recv()
        onward_share(v, i).start()

    def shared(v, slot):
        ref, sem = win.at[v, slot, 1 - half], (pr, qr)[slot - 1]
        remote(ref, ref, wins.at[v], sem.at[v], partner).wait_recv()

    grid_swap, edge_swap = swap(gridv, send.at[0], recv.at[0]), swap(xv, send.at[1], recv.at[1])
    mesh_swap = swap(win.at[0, 0], send.at[2], recv.at[2])
    cot_swap = swap(win.at[1, 0], send.at[3], recv.at[3])

    for copy in loads[:2]:
        copy.wait()
    pl.semaphore_wait(barrier, n)
    for v in (0, 1):
        for i in range(steps):
            pair_copy(v, i).start()
    for copy in loads[2:4]:
        copy.wait()
    for copy in (grid_swap, mesh_swap, edge_swap, cot_swap):
        copy.start()
    for copy in loads[4:]:
        copy.wait()
    wg_t[...] = turned(wgv[...])
    we_t[...] = turned(wev[...])
    bcol = jnp.broadcast_to(biasv[...].reshape(1, hidden), (128, hidden)).T[:, :1]

    block, lanes = 256, 128
    counted = lax.broadcasted_iota(jnp.int32, (block, lanes), 0).astype(F32).astype(BF)
    one, zero = jnp.ones((block, lanes), BF), jnp.zeros((block, lanes), BF)

    def mark(ref, row, cut):
        for base in range(0, ref.shape[0], block):
            size = min(block, ref.shape[0] - base)
            local_row = row - base
            local_row = jnp.where((local_row >= 0) & (local_row < size), local_row, -1)
            local_row = local_row.astype(F32).astype(BF)
            for j in range(0, tile, lanes):
                ref[base:base + size, cut.start + j:cut.start + j + lanes] = jnp.where(
                    counted[:size] == local_row[:, j:j + lanes], one[:size], zero[:size])

    band_row, mesh_row = me * (2 * rows_g), me * own_m
    to_below, to_above = own_m * (3 - odd), own_m * odd
    cuts = [slice(t * tile, (t + 1) * tile) for t in range(tiles)]
    for cut in cuts:
        from_row = senderv[cut].reshape(1, tile) - band_row
        to_row = receiverv[cut].reshape(1, tile) - mesh_row
        to_row = to_row + jnp.where(to_row < 0, to_below, jnp.where(to_row >= own_m, to_above, 0))
        mark(s_t, from_row, cut)
        mark(r_t, to_row, cut)

    grid_swap.wait()
    grid_all = lambda: gridv[...].reshape(2 * rows_g, width)
    pg[...] = mm(wg_t[...], grid_all(), NT).astype(BF)
    pass_pair(0, 0)
    edge_swap.wait()
    x_all = lambda: xv[...].reshape(edges, width)
    for t, cut in enumerate(cuts):
        pre_v[:, cut] = mm(pg[...], s_t[:, cut]) + mm(we_t[...], x_all()[cut], NT) + bcol
        if t == 0:
            for i in range(1, steps):
                pass_pair(0, i)

    near_rows, early = 2 * own_m, padded // 2
    assert early <= near_rows

    def nodes(which):
        rows_in = win[which].reshape(window, width)
        if padded > window:
            rows_in = jnp.concatenate(
                [rows_in, jnp.zeros((padded - window, width), BF)], axis=0)
        return rows_in

    def near_nodes(which):
        return win[which, :2].reshape(near_rows, width)

    def last_nodes(which):
        return jnp.concatenate([
            win[which, 2].reshape(own_m, width),
            jnp.zeros((padded - window, width), BF)], axis=0)

    for i in range(steps // 2):
        pass_pair(1, i)
    mesh_swap.wait()
    shared(0, 1)
    pm[:, :near_rows] = mm(near_nodes(0), wmv[...]).T.astype(BF)
    for t, cut in enumerate(cuts):
        pre_v[:, cut] += mm(pm[:, :early], r_t[:early, cut])
        if t == tiles - 2:
            pass_onward(0, 0)
            for i in range(steps // 2, steps):
                pass_pair(1, i)
    for i in range(1, steps):
        pass_onward(0, i)
    cot_swap.wait()
    shared(1, 1)
    pc[:, :near_rows] = mm(wov[...], near_nodes(1), NT).astype(BF)
    for cut in cuts:
        hid_v[:, cut] = mm(pc[:, :early], r_t[:early, cut])
    shared(0, 2)
    pm[:, near_rows:] = mm(last_nodes(0), wmv[...]).T.astype(BF)
    count = used[0]
    alive = [
        jnp.where(lax.broadcasted_iota(jnp.int32, (1, tile), 1) + t * tile < count, 1.0, 0.0)
        for t in range(tiles)
    ]
    later = list(range(steps))
    for t, cut in enumerate(cuts):
        pre = pre_v[:, cut] + mm(pm[:, early:], r_t[early:, cut])
        sig = jax.nn.sigmoid(pre)
        act_v[:, cut] = (pre * sig * alive[t]).astype(BF)
        pre_v[:, cut] = sig * (1.0 + pre * (1.0 - sig)) * alive[t]
        if t == 0:
            pass_onward(1, 0)
    for i in range(1, steps):
        pass_onward(1, i)
    rsum[...] = mm(act_v[...], r_t[...], NT).astype(BF)
    shared(1, 2)

    sign = 1 - 2 * (plane // (high // 2))
    far = lambda k: lax.rem(plane + sign * k + high, high)
    turn = lambda bit, k: 1 - bits[bit] if (k >> bit) & 1 else bits[bit]
    near = lambda k: turn(0, k) + 2 * turn(1, k)
    peer = lambda k: at(plane * 4 + near(k))
    distant = lambda k: at(far(k) * 4 + mine)

    def to(stage, w, c, src, dst, device):
        remote(src, dst, ws.at[w, c], wr.at[stage, w, c], device).start()

    def landed(stage, w, c, ref):
        remote(ref, ref, ws.at[w, c], wr.at[stage, w, c], partner).wait()

    def offer(w, value):
        part = width // cuts_w
        for c in range(cuts_w):
            gall[w, c] = value[:, c * part:(c + 1) * part].reshape(gall.shape[2:]).astype(BF)
            for k in (3, 1, 2):
                to(0, w, c, gall.at[w, c, near(k)], in1.at[w, c, k], peer(k))

    def step1(w, c):
        landed(0, w, c, in1.at[w, c, pl.ds(1, 3)])
        total = gall[w, c, mine].astype(F32)
        for k in range(1, 4):
            total = total + in1[w, c, k].astype(F32)
        sum1[w, c] = total.astype(BF)
        each(1, high, lambda k: to(
            1, w, c, sum1.at[w, c, far(high - k)], in2.at[w, c, plane], distant(high - k)))

    def step2(w, c):
        landed(1, w, c, in2.at[w, c, pl.ds(1, high - 1)])
        in2[w, c, plane] = sum1[w, c, plane]
        sum2[w, c] = jnp.sum(in2[w, c].astype(F32), axis=0).astype(BF)
        each(1, high, lambda k: to(
            2, w, c, sum2.at[w, c], out1.at[w, c, plane], distant(high - k)))
        out1[w, c, plane] = sum2[w, c]

    def step3(w, c):
        landed(2, w, c, in2.at[w, c, pl.ds(1, high - 1)])
        if w in SPLIT:
            to(3, w, c, out1.at[w, c], in1.at[w, c, 0], along(second(c)))
        else:
            for k in (3, 1, 2):
                to(3, w, c, out1.at[w, c], out.at[w, c, mine], peer(k))
        keep(w, c).start()

    def step4(w, c):
        if w in SPLIT:
            landed(3, w, c, in1.at[w, c, 0])
            to(4, w, c, out1.at[w, c], out.at[w, c, mine], along(first(c)))
            to(4, w, c, in1.at[w, c, 0], out.at[w, c, flipped(second(c))], along(first(c)))
            keep_landed(w, c).start()
        else:
            landed(3, w, c, in1.at[w, c, pl.ds(1, 3)])

    def step5(w, c):
        if w in SPLIT:
            landed(4, w, c, in1.at[w, c, pl.ds(1, 2)])

    first = lambda c: c % 2
    second = lambda c: 1 - c % 2
    shift = lambda bit: (1 - 2 * bits[bit]) * (1 + bit)
    along = lambda bit: at(me + shift(bit))
    flipped = lambda bit: mine + shift(bit)

    def keep_landed(w, c):
        return pltpu.make_async_copy(
            in1.at[w, c, 0], out.at[w, c, flipped(second(c))], local.at[14])

    def keep(w, c):
        return pltpu.make_async_copy(out1.at[w, c], out.at[w, c, mine], local.at[15])

    stages = (step1, step2, step3, step4, step5)

    def bias_low(k):
        return remote(gb_own, gb_in.at[k], send.at[4], recv.at[4], peer(k))

    def bias_high(k):
        return remote(gb_sum, gb_all.at[plane], send.at[5], recv.at[5], distant(k))

    parts = range(rx.shape[1])
    rx_on = [
        remote(rx.at[2, i], rims.at[0, i], send.at[9 + i], recv.at[9 + i], at(backward))
        for i in parts
    ]
    rx_pair = [
        remote(rxs.at[i], rims.at[1, i], send.at[3 + 10 + i], recv.at[3 + 10 + i], at(pair))
        for i in parts
    ]
    grid_copy = remote(gg_v.at[1 - half], gg_in, send.at[6], recv.at[6], partner)
    edge_copy = remote(ge_v.at[1 - half], ge_in, send.at[7], recv.at[7], partner)
    mesh_copy = remote(gm_v.at[1 - half], gm_in, send.at[8], recv.at[8], partner)

    def settle(copy, own, other, to, i):
        copy.wait()
        own[half] = (own[half].astype(F32) + other[...].astype(F32)).astype(BF)
        pltpu.make_async_copy(own.at[half], to, local.at[i]).start()

    grid_sum = (grid_copy, gg_v, gg_in, grid_out, 11)
    edge_sum = (edge_copy, ge_v, ge_in, edge_out, 12)
    mesh_sum = (mesh_copy, gm_v, gm_in, mesh_out, 13)
    bias_done = pltpu.make_async_copy(gb_out, bias_out, local.at[16])

    def rx_step1(i):
        rx_on[i].wait()
        rxs[i] = (rx[1, i].astype(F32) + rims[0, i].astype(F32)).astype(BF)
        rx_pair[i].start()

    def rx_step2():
        for copy in rx_pair:
            copy.wait()
        total = (rx[0].astype(F32) + rims[1].astype(F32)).astype(BF).reshape(own_m, hidden)
        gm_v[...] = mm(total, wmv[...], NT).astype(BF).reshape(gm_v.shape)
        mesh_copy.start()

    def bias_step1():
        ref = gb_in.at[pl.ds(1, 3)]
        remote(ref, ref, send.at[4], recv.at[4], partner).wait()
        gb_in[0] = gb_own[...]
        gb_sum[...] = jnp.sum(gb_in[...], axis=0)
        each(1, high, lambda k: bias_high(k).start())

    def bias_step2():
        ref = gb_all.at[pl.ds(1, high - 1)]
        remote(ref, ref, send.at[5], recv.at[5], partner).wait()
        gb_all[plane] = gb_sum[...]
        gb_out[...] = jnp.sum(gb_all[...], axis=0)
        bias_done.start()

    def make_wo():
        offer(WO, mm(rsum[...], nodes(1)))

    def make_hidden():
        pc[:, near_rows:] = mm(wov[...], last_nodes(1), NT).astype(BF)
        for cut in cuts:
            hidden_cot = hid_v[:, cut] + mm(pc[:, early:], r_t[early:, cut])
            pc_v[:, cut] = (hidden_cot * pre_v[:, cut]).astype(BF)

    def make_we():
        offer(WE, mm(pc_v[...], x_all()))

    def make_bias():
        gb = jnp.zeros((hidden, 128), F32)
        for k in range(edges // 128):
            gb = gb + pc_v[:, k * 128:(k + 1) * 128].astype(F32)
        gb_own[...] = jnp.broadcast_to(jnp.sum(gb.T, axis=0, keepdims=True), gb_own.shape)
        for k in range(1, 4):
            bias_low(k).start()

    def make_wm():
        sr = mm(pc_v[...], r_t[...], NT)
        offer(WM, mm(sr.astype(BF), nodes(0)))
        rx[...] = sr.T[:window].astype(BF).reshape(rx.shape)

    split = rows_g // 128 * 128 + 128

    def make_sg():
        sg[:, :split] = mm(pc_v[...], s_t[:split], NT).astype(BF)

    def make_wg():
        sg[:, split:] = mm(pc_v[...], s_t[split:], NT).astype(BF)
        offer(WG, mm(sg[...], grid_all()))

    def make_grid():
        gg_v[...] = mm(sg[...], wg_t[...], TN).astype(BF).reshape(gg_v.shape)
        grid_copy.start()

    def make_edge():
        ge_v[...] = mm(pc_v[...], we_t[...], TN).astype(BF).reshape(ge_v.shape)
        edge_copy.start()

    PLAN = (
        (11.1, "rx0a", lambda now: rx_on[0].start()),
        (15.6, "rx1a", lambda now: rx_step1(0)),
        (12.5, "rx0b", lambda now: rx_on[1].start()),
        (16.6, "rx1b", lambda now: rx_step1(1)),
        (13.6, "rx0c", lambda now: rx_on[2].start()),
        (17.8, "rx1c", lambda now: rx_step1(2)),
        (15.0, "rx0d", lambda now: rx_on[3].start()),
        (19.0, "rx1d", lambda now: rx_step1(3)),
        (15.0, "bias1", lambda now: bias_step1()),
        (12.2, "set_grid", lambda now: settle(*grid_sum)),
        (12.3, "set_edge", lambda now: settle(*edge_sum)),
        (24.5, "rx2", lambda now: rx_step2()),
        (26.5, "set_mesh", lambda now: settle(*mesh_sum)),
        (21.5, "bias2", lambda now: bias_step2()),
    )
    events = []

    def plan(time, name, fn):
        events.append((time, len(events), name, fn))

    def chain(time, w, c):
        for fn, lasts in zip(stages, STAGE):
            time = time + lasts + (1.5 if fn is step4 and w not in SPLIT else 0.0)
            plan(time, f"{fn.__name__}_{w}{c}", lambda now, fn=fn: fn(w, c))

    def due(now):
        while events and min(events)[0] <= now:
            event = min(events)
            events.remove(event)
            event[3](max(now, event[0]) if now < 1e6 else event[0])

    def offered(w):
        return lambda now: [
            chain(max(now + 2.2, 2.65) + 1.4 * (c + 1) + 0.8 * w, w, c) for c in range(cuts_w)]

    now = 0.0
    for name, fn, lasts, after in (
        ("gwo", make_wo, 0.45, offered(WO)),
        ("hid", make_hidden, 1.2, None),
        ("gwe", make_we, 0.8, offered(WE)),
        ("sr", make_wm, 1.95, offered(WM)),
        ("sg", make_sg, 1.3, None),
        ("gwg", make_wg, 1.3, offered(WG)),
        ("bias", make_bias, 0.2, None),
        ("gradgrid", make_grid, 0.5, None),
        ("gradedge", make_edge, 0.8, None),
    ):
        due(now)
        fn()
        now += lasts
        if after is not None:
            after(now)
    for time, name, fn in PLAN:
        plan(time, name, fn)
    due(1e9)
    for copy, own, _, to, i in (grid_sum, edge_sum, mesh_sum):
        pltpu.make_async_copy(own.at[half], to, local.at[i]).wait()
    bias_done.wait()
    pltpu.make_async_copy(out1, out1, local.at[15]).wait()
    for v in (0, 1):
        ref = win.at[v, pl.ds(0, 2)]
        remote(ref, ref, wins.at[v], pr.at[v], partner).wait_send()


def final_kernel(
    grid_sum, edge_sum, mesh_sum, out, bias_sum,
    grad_grid, grad_edge, grad_mesh, gwg, gwm, gwe, gbias, gwo,
    gv, ev, mv, outv, bv, wide, tall, flat, came, went,
):
    rows = ev.shape[0] // 2
    halves = [pl.ds(i * rows, rows) for i in (0, 1)]
    passing = [
        (edge_sum.at[halves[0]], ev.at[halves[0]], grad_edge.at[halves[0]]),
        (edge_sum.at[halves[1]], ev.at[halves[1]], grad_edge.at[halves[1]]),
        (grid_sum, gv, grad_grid), (mesh_sum, mv, grad_mesh),
    ]
    copy = pltpu.make_async_copy
    into = [copy(out.at[w], outv.at[w], came.at[w]) for w in range(4)]
    into.append(copy(bias_sum, bv, came.at[8]))
    take = [copy(src, mid, came.at[4 + i]) for i, (src, mid, _) in enumerate(passing)]
    give = [copy(mid, dst, went.at[4 + i]) for i, (_, mid, dst) in enumerate(passing)]
    done = [
        copy(wide, gwo, went.at[WO]), copy(tall.at[0], gwe, went.at[WE]),
        copy(tall.at[1], gwm, went.at[WM]), copy(tall.at[2], gwg, went.at[WG]),
    ]
    for read in (into[0], take[0], into[1], take[1], into[2], take[2], into[3], take[3], into[4]):
        read.start()
    for w in range(4):
        into[w].wait()
        value = jnp.concatenate([
            outv[w, c].astype(F32).reshape(wide.shape[0], -1) for c in range(outv.shape[1])
        ], axis=1)
        if w == WO:
            wide[...] = value
        else:
            tall[w - 1] = value.T
        done[w].start()
        take[w].wait()
        give[w].start()
    into[4].wait()
    flat[...] = bv[...][0]
    last = copy(flat, gbias, went.at[8])
    last.start()
    for write in done + give + [last]:
        write.wait()


def body(
    grid_latent,
    edge_latent,
    mesh_latent,
    mesh_cotangent,
    w_grid,
    w_mesh,
    w_edge,
    bias,
    w_out,
    senders,
    receivers,
    edge_count,
):
    n = lax.axis_size("band")
    rows_g, width = grid_latent.shape
    rows_e = edge_latent.shape[0]
    rows_m = mesh_latent.shape[0]
    hidden = w_grid.shape[1]
    own_m = 2 * rows_m
    edges = 2 * rows_e
    sds = jax.ShapeDtypeStruct
    dma = pltpu.SemaphoreType.DMA
    vm = pltpu.VMEM

    tile = max(d for d in range(128, 1025, 128) if edges % d == 0)
    padded = -(-3 * own_m // 256) * 256
    high = n // 4
    rows_c = hidden // n
    cuts_w, steps = 2, 2
    piece = (rows_c, width // cuts_w)
    rim = (4, own_m // 4, hidden)
    edge_sum, grid_sum, mesh_sum, out, bias_sum = pl.pallas_call(
        functools.partial(mega_kernel, tile),
        out_shape=(
            sds((rows_e, width), BF), sds((rows_g, width), BF), sds((rows_m, width), BF),
            sds((4, cuts_w, 4, high) + piece, BF), sds((8, hidden), F32),
        ),
        in_specs=[pl.BlockSpec(memory_space=pltpu.SMEM)] + [ANY] * 11,
        out_specs=(ANY,) * 5,
        scratch_shapes=[
            vm((2, rows_g, width), BF), vm((2, rows_e, width), BF),
            vm((2, 3, 2, steps, rows_m // steps, width), BF),
            vm((width, hidden), BF), vm((width, hidden), BF), vm((width, hidden), BF),
            vm((hidden, width), BF), vm((hidden,), F32),
            vm((edges,), jnp.int32), vm((edges,), jnp.int32),
            vm((hidden, width), BF), vm((hidden, width), BF),
            vm((2 * rows_g, edges), BF), vm((padded, edges), BF),
            vm((hidden, 2 * rows_g), BF), vm((hidden, padded), BF), vm((hidden, padded), BF),
            vm((hidden, edges), F32), vm((hidden, edges), F32), vm((hidden, edges), BF), vm((hidden, edges), BF),
            vm((hidden, 2 * rows_g), BF),
            vm((hidden, padded), BF),
            vm((2, rows_e, width), BF), vm((rows_e, width), BF),
            vm((2, rows_g, width), BF), vm((rows_g, width), BF),
            vm((3,) + rim, BF), vm((2,) + rim, BF), vm(rim, BF),
            vm((2, rows_m, width), BF), vm((rows_m, width), BF),
            vm((4, cuts_w, 4, high) + piece, BF), vm((4, cuts_w, 4, high) + piece, BF),
            vm((4, cuts_w, high) + piece, BF), vm((4, cuts_w, high) + piece, BF),
            vm((4, cuts_w) + piece, BF), vm((4, cuts_w, high) + piece, BF),
            vm((8, hidden), F32), vm((4, 8, hidden), F32), vm((8, hidden), F32),
            vm((high, 8, hidden), F32), vm((8, hidden), F32),
            dma((17,)), dma((17,)), dma((17,)),
            dma((2,)), dma((2, steps)), dma((2, steps)), dma((2,)), dma((2,)),
            dma((4, cuts_w)), dma((5, 4, cuts_w)),
        ],
        compiler_params=pltpu.CompilerParams(
            collective_id=0, has_side_effects=True, vmem_limit_bytes=60 * 2**20),
    )(
        edge_count, grid_latent, edge_latent, mesh_latent, mesh_cotangent,
        w_grid, w_edge, w_mesh, w_out, bias, senders, receivers,
    )

    return pl.pallas_call(
        final_kernel,
        in_specs=[ANY] * 5,
        out_specs=(ANY,) * 8,
        out_shape=(
            sds((rows_g, width), BF), sds((rows_e, width), BF), sds((rows_m, width), BF),
            sds((width, hidden), F32), sds((width, hidden), F32), sds((width, hidden), F32),
            sds((hidden,), F32), sds((hidden, width), F32),
        ),
        scratch_shapes=[
            vm((rows_g, width), BF), vm((rows_e, width), BF), vm((rows_m, width), BF),
            vm((4, cuts_w, n) + piece, BF), vm((8, hidden), F32),
            vm((hidden, width), F32), vm((3, width, hidden), F32), vm((hidden,), F32),
            dma((9,)), dma((9,)),
        ],
    )(grid_sum, edge_sum, mesh_sum, out.reshape((4, cuts_w, n) + piece), bias_sum)


def solution(mesh):
    rows = P(("band", "chan"), None)
    return jax.shard_map(
        body,
        mesh=mesh,
        in_specs=(
            rows, rows, rows, rows,
            P(None, "chan"), P(None, "chan"), P(None, "chan"), P("chan"), P("chan", None),
            P("band"), P("band"), P("band"),
        ),
        out_specs=(
            rows, rows, rows,
            P(None, "chan"), P(None, "chan"), P(None, "chan"), P("chan"), P("chan", None),
        ),
        check_vma=False,
    )
```
